32 devices in a mesh: dp: 2 (over x), tp: 16 (over y, z, core).
Axes of the slice: x: 2, y: 2, z: 4, core: 2. Of those that a mesh axis runs over, the one named last changes fastest.
Arguments:
- x: bfloat16 [8192, 4096], P(('dp', 'tp')), parts along dimension 0
- dy: bfloat16 [8192, 4096], P(('dp', 'tp')), parts along dimension 0
- gain: bfloat16 [4096], replicated
- wq: bfloat16 [4096, 4096], P(None, 'tp')
- wk: bfloat16 [4096, 4096], P(None, 'tp')
- wv: bfloat16 [4096, 4096], P(None, 'tp')
- wo: bfloat16 [4096, 4096], P('tp')
Outputs:
- output 1: bfloat16 [8192, 4096], P(('dp', 'tp')), parts along dimension 0
- output 2: float32 [2, 4096], P('dp'), parts along dimension 0
- output 3: bfloat16 [8192, 4096], P('dp', 'tp'), parts along dimension 0
- output 4: bfloat16 [8192, 4096], P('dp', 'tp'), parts along dimension 0
- output 5: bfloat16 [8192, 4096], P('dp', 'tp'), parts along dimension 0
- output 6: bfloat16 [8192, 4096], P(('dp', 'tp')), parts along dimension 0
There are 2 independent parts. The reference program is written for one: setup_inputs(seed, part) draws one part's arguments, and reference() takes and returns one part's arrays. A program takes and returns all parts, laid end to end along the dimension named above; an argument that names none is the same for every part.
All inputs are finite; a program needn't handle non-finite values.
Results may differ from the reference program's by a relative error of at most 0.018.
Values are sent between devices in bfloat16 or wider.
A program may use at most 2 GiB of HBM per device.

```python
import jax
import jax.numpy as jnp
from jax import lax

ROWS = 4096
D = 4096
HEADS = 32
KV_HEADS = 32
HEAD = 128
THETA = 10000


def setup_inputs(seed: int = 0, part: int = 0) -> dict:
    kx, ky, kn, kq, kk, kv, ko = jax.random.split(jax.random.key(seed), 7)

    def weights(key, rows, columns):
        return jax.random.normal(key, (rows, columns), jnp.float32) * rows**-0.5

    drawn = {
        "x": jax.random.normal(jax.random.fold_in(kx, part), (ROWS, D), jnp.float32),
        "dy": jax.random.normal(jax.random.fold_in(ky, part), (ROWS, D), jnp.float32) * ROWS**-0.5,
        "gain": 1 + 0.1 * jax.random.normal(kn, (D,), jnp.float32),
        "wq": 2 * weights(kq, D, HEADS * HEAD),
        "wk": 2 * weights(kk, D, KV_HEADS * HEAD),
        "wv": 4 * weights(kv, D, KV_HEADS * HEAD),
        "wo": weights(ko, HEADS * HEAD, D),
    }
    return {k: v.astype(jnp.bfloat16) for k, v in drawn.items()}


def normed(x, gain):
    wide = x.astype(jnp.float32)
    scale = lax.rsqrt(jnp.mean(wide * wide, -1, keepdims=True) + 1e-6)
    return (wide * scale * gain.astype(jnp.float32)).astype(jnp.bfloat16)


def turned(t, place, theta):
    half = t.shape[-1] // 2
    angle = place.astype(jnp.float32)[:, None] * theta ** (-jnp.arange(half, dtype=jnp.float32) / half)
    cos, sin = jnp.cos(angle)[:, None], jnp.sin(angle)[:, None]
    a, b = t[..., :half].astype(jnp.float32), t[..., half:].astype(jnp.float32)
    return jnp.concatenate([a * cos - b * sin, b * cos + a * sin], -1).astype(jnp.bfloat16)


def matmul(a, w):
    return jnp.dot(a, w, preferred_element_type=jnp.float32).astype(jnp.bfloat16)


def einsum(form, a, b):
    return jnp.einsum(form, a.astype(jnp.float32), b.astype(jnp.float32))


def attention(q, k, v):
    scores = einsum("tgsd,ugd->gstu", q, k) * q.shape[-1] ** -0.5
    token = jnp.arange(q.shape[0])
    scores = jnp.where(token[:, None] >= token, scores, -jnp.inf)
    weights = jax.nn.softmax(scores, -1).astype(jnp.bfloat16)
    return einsum("gstu,ugd->tgsd", weights, v).astype(jnp.bfloat16)


def forward(x, gain, wq, wk, wv, wo):
    rows = x.shape[0]
    a, place = normed(x, gain), jnp.arange(rows)
    k = turned(matmul(a, wk).reshape(rows, -1, HEAD), place, THETA)
    q = turned(matmul(a, wq).reshape(rows, -1, HEAD), place, THETA).reshape(rows, k.shape[1], -1, HEAD)
    v = matmul(a, wv).reshape(rows, -1, HEAD)
    seen = attention(q, k, v).reshape(rows, -1)
    return (x.astype(jnp.float32) + jnp.dot(seen, wo, preferred_element_type=jnp.float32)).astype(jnp.bfloat16)


def reference(x, dy, gain, wq, wk, wv, wo):
    _, back = jax.vjp(forward, x, gain.astype(jnp.float32), wq, wk, wv, wo)
    by_x, by_gain, *by_weights = back(dy)
    return (by_x, by_gain[None], *by_weights)
```

```python
import functools

import jax
import jax.numpy as jnp
import numpy as np
from jax import lax
from jax.experimental import pallas as pl
from jax.experimental.pallas import tpu as pltpu
from jax.sharding import PartitionSpec as P

NEG = -1e30
HIDDEN = 2 * NEG
LOG2E = 1.4426950408889634
VMEM = 62 * 2**20
STRIP = 512
KEYS = 512
HEAD = 128
THETA = 10000
ANGLES = 128
EPS = 1e-6
MESH = pl.DeviceIdType.MESH
ANY = pl.BlockSpec(memory_space=pl.ANY)
LOW = jnp.bfloat16
F32 = jnp.float32


def _dot(a, b, ca, cb):
    return lax.dot_general(a, b, (((ca,), (cb,)), ((), ())), preferred_element_type=F32)


def _gap(bk, bq):
    return lax.broadcasted_iota(jnp.int32, (bk, bq), 1) - lax.broadcasted_iota(jnp.int32, (bk, bq), 0)


def _head(i):
    return slice(i * HEAD, (i + 1) * HEAD)


def _pieces(heads, bq):
    return [(i, slice(at, at + STRIP)) for i in range(heads) for at in range(0, bq, STRIP)]


def _cost(rows, width, matmuls):
    return pl.CostEstimate(flops=rows * rows * width * matmuls, transcendentals=rows * rows, bytes_accessed=rows * width * 12)


def _angle(m, far, near):
    here = pl.ds(m, 1)
    cos = far[0, here, :] * near[0] - far[1, here, :] * near[1]
    sin = far[1, here, :] * near[0] + far[0, here, :] * near[1]
    return cos, jnp.where(lax.broadcasted_iota(jnp.int32, sin.shape, 1) < HEAD // 2, sin, -sin)


def _turn(t, angle, way):
    cos, sin = angle
    t = t.astype(LOW).astype(F32)
    swapped = pltpu.roll(t, HEAD // 2, 1) * sin
    return (t * cos + (swapped if way else -swapped)).astype(LOW)


def _backward(q_ref, k_ref, v_ref, do_ref, o_ref, lse_ref, far_ref, near_ref, dq_ref, dk_ref, dv_ref, dq_s, dk_s, dv_s, gap_s, *, heads, bq):
    bk, scale = KEYS, HEAD**-0.5
    e = scale * LOG2E
    iq = pl.program_id(0)
    pieces = _pieces(heads, bq)

    @pl.when(iq == 0)
    def _():
        gap_s[...] = _gap(bk, bq)
        dk_s[...] = jnp.zeros_like(dk_s)
        dv_s[...] = jnp.zeros_like(dv_s)

    dq_s[...] = jnp.zeros_like(dq_s)
    lses = lse_ref[...] * LOG2E
    deltas = [(do_ref[:, _head(i)].astype(F32).T * o_ref[_head(i), :].astype(F32)).sum(0, keepdims=True) for i in range(heads)]

    def block(j, masked):
        here = pl.ds(pl.multiple_of(j * bk, bk), bk)
        qs = [q_ref[at, _head(i)] for i, at in pieces]
        dos = [do_ref[at, _head(i)] for i, at in pieces]
        scores = [_dot(k_ref[here, _head(i)], x, 1, 1) for (i, _), x in zip(pieces, qs)]
        dps = [_dot(v_ref[here, _head(i)], x, 1, 1) for (i, _), x in zip(pieces, dos)]
        ok = gap_s[...] >= j * bk - iq * bq if masked else None
        for n, (i, at) in enumerate(pieces):
            p = jnp.exp2(scores[n] * e - lses[i : i + 1, at])
            if masked:
                p = jnp.where(ok[:, at], p, 0.0)
            ds = (p * (dps[n] - deltas[i][:, at])).astype(LOW)
            dv_s[i, here, :] += _dot(p.astype(LOW), dos[n], 1, 0)
            dk_s[i, here, :] += _dot(ds, qs[n], 1, 0)
            dq_s[i, :, at] += _dot(k_ref[here, _head(i)].T, ds, 1, 0)

    whole = iq * (bq // bk)
    lax.fori_loop(0, whole, lambda j, _: block(j, False), None)
    lax.fori_loop(whole, whole + bq // bk, lambda j, _: block(j, True), None)
    for n in range(bq // ANGLES):
        angle, at = _angle(iq * (bq // ANGLES) + n, far_ref, near_ref), slice(n * ANGLES, (n + 1) * ANGLES)
        for i in range(heads):
            dq_ref[at, _head(i)] = _turn((dq_s[i, :, at] * scale).T, angle, 1)

    @pl.when(iq == pl.num_programs(0) - 1)
    def _():
        def finish(j, _):
            here = pl.ds(pl.multiple_of(j * ANGLES, ANGLES), ANGLES)
            angle = _angle(j, far_ref, near_ref)
            for i in range(heads):
                dk_ref[here, _head(i)] = _turn(dk_s[i, here, :] * scale, angle, 1)
                dv_ref[here, _head(i)] = dv_s[i, here, :].astype(LOW)

        lax.fori_loop(0, dk_s.shape[1] // ANGLES, finish, None)


def attend_bwd(q, k, v, d_out, out, lse, far, near):
    rows, width = q.shape
    heads, bq = width // HEAD, 1024
    some, whole = (bq, width), pl.BlockSpec((rows, width), lambda iq: (0, 0))
    tables = [pl.BlockSpec(t.shape, lambda iq: (0, 0, 0)) for t in (far, near)]
    queries = pl.BlockSpec(some, lambda iq: (iq, 0))
    return pl.pallas_call(
        functools.partial(_backward, heads=heads, bq=bq),
        grid=(rows // bq,),
        in_specs=[queries, whole, whole, queries, pl.BlockSpec(some[::-1], lambda iq: (0, iq)), pl.BlockSpec((heads, bq), lambda iq: (0, iq)),
                  *tables],
        out_specs=[queries, whole, whole],
        out_shape=[jax.ShapeDtypeStruct(q.shape, LOW)] * 3,
        scratch_shapes=[pltpu.VMEM((heads, HEAD, bq), F32), pltpu.VMEM((heads, rows, HEAD), F32), pltpu.VMEM((heads, rows, HEAD), F32),
                        pltpu.VMEM((KEYS, bq), jnp.int32)],
        compiler_params=pltpu.CompilerParams(dimension_semantics=("arbitrary",), vmem_limit_bytes=VMEM),
        cost_estimate=_cost(rows, width, 5),
    )(q, k, v, d_out, out, lse, far, near)


GROUP = 16
CHIPS = GROUP // 2
ROWS = 256
STEP = ROWS // 4
BAND = 16


def _ring_chip(place):
    return jnp.where(place < CHIPS // 2, place, CHIPS + CHIPS // 2 - 1 - place)


def _greet(others):
    barrier = pltpu.get_barrier_semaphore()
    for other in others:
        pl.semaphore_signal(barrier, inc=1, device_id={"tp": other}, device_id_type=MESH)
    pl.semaphore_wait(barrier, len(others))


def _scatter(dq_h, dk_h, dv_h, wq_h, wk_h, wv_h, at_h, dy_h, seen_h, x_h, my_dy_h, gain_h, dx_ref, dgain_ref, dwq_h, dwk_h, dwv_h, dwo_h,
             dqkv, w, seen, x_s, my_dy, gain, lhs, own, twin_out, twin_in, ring_out, ring_in, total_s, unit_sum, gain_out, gain_in,
             at_s, dy_s, dw_s, dwo_s,
             load_sem, twin_send, twin_recv, ring_send, ring_recv, gain_send, gain_recv, at_sem, dy_sem, dw_sem, dwo_sem):
    me = lax.axis_index("tp")
    chip, core = me // 2, me % 2
    place = _ring_chip(chip)
    twin = 2 * chip + 1 - core
    after = 2 * _ring_chip((place + 1) % CHIPS) + core
    before = 2 * _ring_chip((place + CHIPS - 1) % CHIPS) + core
    width = w.shape[0]
    part = [slice(n * ROWS, (n + 1) * ROWS) for n in range(3)]

    given = (*((a, dqkv.at[:, here]) for a, here in zip((dq_h, dk_h, dv_h), part)), *((a, w.at[:, here]) for a, here in zip((wq_h, wk_h, wv_h), part)),
             (seen_h, seen), (x_h, x_s), (my_dy_h, my_dy), (gain_h, gain))
    loads = [pltpu.make_async_copy(a, b, load_sem.at[n]) for n, (a, b) in enumerate(given)]
    for load in loads:
        load.start()

    def fetch(u, slot):
        here = pl.ds(pl.multiple_of(u * ROWS, ROWS), ROWS)
        return (pltpu.make_async_copy(at_h.at[here, :], at_s.at[slot], at_sem.at[slot]),
                pltpu.make_async_copy(dy_h.at[1, :, here], dy_s.at[slot], dy_sem.at[slot]))

    def put(u, slot):
        here = pl.ds(pl.multiple_of(u * ROWS, ROWS), ROWS)
        return (*(pltpu.make_async_copy(dw_s.at[slot, n], out.at[here, :], dw_sem.at[slot, n]) for n, out in enumerate((dwq_h, dwk_h, dwv_h))),
                pltpu.make_async_copy(dwo_s.at[slot], dwo_h.at[:, here], dwo_sem.at[slot]))

    for copy in fetch(0, 0):
        copy.start()
    others = [(me + d) % GROUP for d in range(1, GROUP)]
    _greet(others)

    def swap(slot, c):
        return pltpu.make_async_remote_copy(src_ref=twin_out.at[slot, c], dst_ref=twin_in.at[slot, c], send_sem=twin_send.at[slot, c],
                                            recv_sem=twin_recv.at[slot, c], device_id={"tp": twin}, device_id_type=MESH)

    def hop(slot, way, c):
        here = pl.ds(way * STEP, STEP)
        return pltpu.make_async_remote_copy(src_ref=ring_out.at[c, here, :], dst_ref=ring_in.at[slot, c, here, :], send_sem=ring_send.at[way, c],
                                            recv_sem=ring_recv.at[slot, way, c], device_id={"tp": before if way else after}, device_id_type=MESH)

    def terms(s, c):
        forth = _ring_chip((place + 2 * CHIPS - 1 - s) % CHIPS)
        back = _ring_chip((place + 1 + s) % CHIPS)
        starts = [(2 * to + of) * ROWS + (2 * way + c) * STEP for of in (core, 1 - core) for way, to in ((0, forth), (1, back))]
        for n, start in enumerate(starts):
            lhs[n * STEP : (n + 1) * STEP, :] = dqkv[pl.ds(pl.multiple_of(start, STEP), STEP), :]
        slot = s % 2

        def columns(j, _):
            here = pl.ds(pl.multiple_of(j * STRIP, STRIP), STRIP)
            term = _dot(lhs[...], w[here, :], 1, 1)
            own[c, :, here] = term[: 2 * STEP]
            twin_out[slot, c, :, here] = term[2 * STEP :].astype(LOW)

        lax.fori_loop(0, width // STRIP, columns, None)
        swap(slot, c).start()

    def add(s, c, ringed, last):
        slot = s % 2

        def columns(j, _):
            here = pl.ds(pl.multiple_of(j * ROWS, ROWS), ROWS)
            total = own[c, :, here] + twin_in[slot, c, :, here].astype(F32)
            if ringed:
                total += ring_in[1 - slot, c, :, here].astype(F32)
            if last:
                total_s[:, here] = total
            else:
                ring_out[c, :, here] = total.astype(LOW)

        lax.fori_loop(0, width // ROWS, columns, None)

    def norm(c):
        def band(j, _):
            src = pl.ds(pl.multiple_of(j * BAND, BAND), BAND)
            at = c * STEP + j * BAND + jnp.where(j >= STEP // BAND, STEP, 0)
            dst = pl.ds(pl.multiple_of(at, BAND), BAND)
            wide, by = x_s[dst, :].astype(F32), total_s[src, :]
            scale = lax.rsqrt(jnp.mean(wide * wide, -1, keepdims=True) + EPS)
            unit = wide * scale
            unit_sum[...] += by * unit
            by = by * gain[...].astype(F32)
            dx = scale * (by - unit * jnp.mean(by * unit, -1, keepdims=True))
            dx_ref[dst, :] = (my_dy[dst, :].astype(F32) + dx).astype(LOW)

        lax.fori_loop(0, 2 * STEP // BAND, band, None)

    def weights(u, slot):
        for copy in fetch(u, slot):
            copy.wait()

        @pl.when(u < GROUP - 1)
        def _():
            for copy in fetch(u + 1, 1 - slot):
                copy.start()

        @pl.when(u >= 2)
        def _():
            for copy in put(u, slot):
                copy.wait()

        for n in range(3):
            dw_s[slot, n] = _dot(at_s[slot], dqkv[:, part[n]], 1, 0).astype(LOW)
        dwo_s[slot] = _dot(seen[...], dy_s[slot], 1, 0).astype(LOW)
        for copy in put(u, slot):
            copy.start()

    for load in loads[:6]:
        load.wait()
    for c in range(2):
        terms(0, c)
    for load in loads[6:]:
        load.wait()
    unit_sum[...] = jnp.zeros_like(unit_sum)
    last = CHIPS - 1

    def step(s, _):
        slot = s % 2
        for c in range(2):
            swap(slot, c).wait_recv()

            @pl.when(s == 0)
            def _():
                add(s, c, False, False)

            @pl.when(s > 0)
            def _():
                for way in range(2):
                    hop(1 - slot, way, c).wait()
                add(s, c, True, False)

            for way in range(2):
                hop(slot, way, c).start()

            @pl.when(s > 0)
            def _():
                swap(1 - slot, c).wait_send()

            terms(s + 1, c)
            weights(2 * s + c, c)

    lax.fori_loop(0, last, step, None)
    for c in range(2):
        swap(last % 2, c).wait_recv()
        for way in range(2):
            hop(1 - last % 2, way, c).wait()
        add(last, c, True, True)
        norm(c)
        if c == 0:
            weights(2 * last, c)
    gain_out[...] = unit_sum[...].sum(0, keepdims=True)
    gain_in[me] = gain_out[...]
    copies = [pltpu.make_async_remote_copy(src_ref=gain_out, dst_ref=gain_in.at[me], send_sem=gain_send.at[n], recv_sem=gain_recv.at[n],
                                           device_id={"tp": other}, device_id_type=MESH) for n, other in enumerate(others)]
    for copy in copies:
        copy.start()
    weights(2 * last + 1, 1)
    for copy in copies:
        copy.wait()
    dgain_ref[...] = functools.reduce(lambda a, b: a + b, [gain_in[n] for n in range(GROUP)])
    for c in range(2):
        for slot in range(2):
            swap(slot, c).wait_send()
        for copy in put(2 * last + c, c):
            copy.wait()


def scatter(dq, dk, dv, wq, wk, wv, at, dy, seen, x, my_dy, gain):
    width, rows = at.shape
    vmem, dma = pltpu.VMEM, pltpu.SemaphoreType.DMA
    here = pl.BlockSpec(memory_space=pltpu.VMEM)
    part, mine = 2 * STEP, (ROWS, width)
    by_weight = jax.ShapeDtypeStruct((width, ROWS), LOW)
    return pl.pallas_call(
        _scatter,
        in_specs=[ANY] * 12,
        out_specs=[here] * 2 + [ANY] * 4,
        out_shape=[jax.ShapeDtypeStruct(mine, LOW), jax.ShapeDtypeStruct((1, width), F32)] + [by_weight] * 3 + [jax.ShapeDtypeStruct(mine, LOW)],
        scratch_shapes=[
            vmem((rows, 3 * ROWS), LOW), vmem((width, 3 * ROWS), LOW), vmem(seen.shape, LOW), vmem(mine, LOW), vmem(mine, LOW), vmem((1, width), LOW),
            vmem((4 * STEP, 3 * ROWS), LOW),
            vmem((2, part, width), F32), vmem((2, 2, part, width), LOW), vmem((2, 2, part, width), LOW),
            vmem((2, part, width), LOW), vmem((2, 2, part, width), LOW), vmem((part, width), F32), vmem((BAND, width), F32),
            vmem((1, width), F32), vmem((GROUP, 1, width), F32),
            vmem((2, ROWS, rows), LOW), vmem((2, rows, ROWS), LOW), vmem((2, 3, ROWS, ROWS), LOW), vmem((2, ROWS, ROWS), LOW),
            dma((10,)), dma((2, 2)), dma((2, 2)), dma((2, 2)), dma((2, 2, 2)), dma((GROUP - 1,)), dma((GROUP - 1,)),
            dma((2,)), dma((2,)), dma((2, 3)), dma((2,)),
        ],
        compiler_params=pltpu.CompilerParams(collective_id=0, has_side_effects=True, vmem_limit_bytes=VMEM),
        cost_estimate=pl.CostEstimate(flops=2 * rows * width * ROWS * 7, transcendentals=0, bytes_accessed=rows * width * 6),
    )(dq, dk, dv, wq, wk, wv, at, dy, seen, x, my_dy, gain)


def tables(rows):
    half = HEAD // 2
    rate = float(THETA) ** (-(np.arange(HEAD) % half) / half)
    turns = [np.arange(0, rows, ANGLES)[:, None] * rate, np.arange(ANGLES)[:, None] * rate]
    return [jnp.asarray(np.stack([np.cos(t), np.sin(t)]), F32) for t in turns]


HALF = ROWS // 2
SPAN = 4 * HALF
QUERIES = 1024


def _gather(x_h, dy_h, gain, wq_h, wk_h, wv_h, wo_h, far, near, all_h, at_h, q_h, k_h, v_h, by_h, out_h, lse_h,
            x_s, mine, w, wo, lhs, turned_s, q, k, v, by, out, lse, top_s, mix_s, gap_s,
            load_sem, store_sem, hop_send, hop_recv, swap_send, swap_recv, lhs_sem, at_sem, result_sem):
    me = lax.axis_index("tp")
    chip, core = me // 2, me % 2
    place = _ring_chip(chip)
    twin = 2 * chip + 1 - core
    ways = [2 * _ring_chip((place + d) % CHIPS) + core for d in (1, CHIPS - 1)]
    barrier = pltpu.get_barrier_semaphore()
    for other in (twin, *ways):
        pl.semaphore_signal(barrier, inc=1, device_id={"tp": other}, device_id_type=MESH)
    part = [slice(n * ROWS, (n + 1) * ROWS) for n in range(3)]
    width = x_s.shape[1]
    heads, bq, bk, scale = ROWS // HEAD, QUERIES, KEYS, HEAD**-0.5
    e = scale * LOG2E

    given = ((x_h, x_s), (dy_h, lhs.at[0, :ROWS, :]), *((a, w.at[:, here]) for a, here in zip((wq_h, wk_h, wv_h), part)), (wo_h, wo))
    loads = [pltpu.make_async_copy(a, b, load_sem.at[n]) for n, (a, b) in enumerate(given)]
    for load in loads:
        load.start()
    here = pl.ds(pl.multiple_of(me * ROWS, ROWS), ROWS)
    stores = [pltpu.make_async_copy(a, all_h.at[n, here, :], store_sem.at[n]) for n, a in enumerate((mine, lhs.at[0, :ROWS, :]))]
    loads[0].wait()

    def norm(j, _):
        band = pl.ds(pl.multiple_of(j * BAND, BAND), BAND)
        wide = x_s[band, :].astype(F32)
        mine[band, :] = (wide * lax.rsqrt(jnp.mean(wide * wide, -1, keepdims=True) + EPS) * gain[...].astype(F32)).astype(LOW)

    lax.fori_loop(0, ROWS // BAND, norm, None)
    stores[0].start()
    loads[1].wait()
    stores[1].start()
    gap_s[...] = _gap(bk, bq)
    for store in stores:
        store.wait()
    for load in loads[2:]:
        load.wait()
    pl.semaphore_wait(barrier, 3)

    def begins(way, g):
        return _ring_chip((place + (g if way else 2 * CHIPS - g)) % CHIPS)

    def piece(p, g, way, c, of):
        start = (2 * begins(way, g) + of) * ROWS + way * HALF + c * STEP
        return all_h.at[p, pl.ds(pl.multiple_of(start, STEP), STEP), :]

    def hop(p, g, way, c):
        rows = piece(p, g, way, c, core)
        return pltpu.make_async_remote_copy(src_ref=rows, dst_ref=rows, send_sem=hop_send.at[p, g, way, c], recv_sem=hop_recv.at[p, g, way, c],
                                            device_id={"tp": ways[way]}, device_id_type=MESH)

    def arrival(p, g, way, c):
        rows = piece(p, g, way, c, core)
        return pltpu.make_async_remote_copy(src_ref=rows, dst_ref=rows, send_sem=hop_send.at[p, g - 1, way, c],
                                            recv_sem=hop_recv.at[p, g - 1, way, c], device_id={"tp": ways[way]}, device_id_type=MESH)

    def swap(p, g, way, c, of):
        rows = piece(p, g, way, c, of)
        return pltpu.make_async_remote_copy(src_ref=rows, dst_ref=rows, send_sem=swap_send.at[p, g, way, c], recv_sem=swap_recv.at[p, g, way, c],
                                            device_id={"tp": twin}, device_id_type=MESH)

    def starts(g):
        return [(2 * begins(way, g) + of) * ROWS + way * HALF for of in (core, 1 - core) for way in range(2)]

    def fetch(n):
        return [pltpu.make_async_copy(all_h.at[n // CHIPS, pl.ds(pl.multiple_of(start, HALF), HALF), :],
                                      lhs.at[n % 2, i * HALF : (i + 1) * HALF, :], lhs_sem.at[n % 2, i]) for i, start in enumerate(starts(n % CHIPS))]

    def put(g):
        return [pltpu.make_async_copy(turned_s.at[:, i * HALF : (i + 1) * HALF], at_h.at[:, pl.ds(pl.multiple_of(start, HALF), HALF)], at_sem.at[i])
                for i, start in enumerate(starts(g))]

    def project(n):
        begin = starts(n % CHIPS)
        for m, to in enumerate((q, k, v)):
            got = _dot(lhs[n % 2], w[:, part[m]], 1, 0).astype(LOW)
            for i, start in enumerate(begin):
                rows = pl.ds(pl.multiple_of(start, HALF), HALF)
                angle = _angle(start // ANGLES, far, near)
                for h in range(heads):
                    t = got[i * HALF : (i + 1) * HALF, _head(h)]
                    to[rows, _head(h)] = t if m == 2 else _turn(t, angle, 0)

    def turn_over(n):
        @pl.when(n > 0)
        def _():
            for copy in put(n - 1):
                copy.wait()

        def columns(j, _):
            here = pl.ds(pl.multiple_of(j * STRIP, STRIP), STRIP)
            turned_s[here, :] = lhs[n % 2, :, here].T

        lax.fori_loop(0, width // STRIP, columns, None)
        for copy in put(n):
            copy.start()

    def products(n):
        got = _dot(lhs[n % 2], wo[...], 1, 1).astype(LOW)
        for i, start in enumerate(starts(n % CHIPS)):
            by[pl.ds(pl.multiple_of(start, HALF), HALF), :] = got[i * HALF : (i + 1) * HALF, :]

    def block(iq, j, masked):
        ones = jnp.ones((8, bk), LOW)
        keys = pl.ds(pl.multiple_of(j * bk, bk), bk)
        pieces = _pieces(heads, bq)
        asked = [pl.ds(pl.multiple_of(iq * bq + at.start, STRIP), STRIP) for _, at in pieces]
        scores = [_dot(k[keys, _head(i)], q[rows, _head(i)], 1, 1) for (i, _), rows in zip(pieces, asked)]
        ok = gap_s[...] >= j * bk - iq * bq if masked else None
        weights, keeps = [], []
        for (i, at), s in zip(pieces, scores):
            if masked:
                s = jnp.where(ok[:, at], s, HIDDEN)
            old = top_s[i : i + 1, at]
            top = jnp.maximum(old, s.max(axis=0, keepdims=True))
            top_s[i : i + 1, at] = top
            weights.append(jnp.exp2((s - top) * e).astype(LOW))
            keeps.append(jnp.exp2((old - top) * e))
        for (i, at), p, keep in zip(pieces, weights, keeps):
            values = jnp.concatenate([v[keys, _head(i)].T, ones], axis=0)
            mix_s[i, :, at] = mix_s[i, :, at] * keep + _dot(values, p, 1, 0)

    per = bq // bk
    count = width // bq
    total = per * count * (count + 1) // 2

    def attend(n):
        iq = sum((n >= per * i * (i + 1) // 2).astype(jnp.int32) for i in range(1, count))
        j = n - per * iq * (iq + 1) // 2

        @pl.when(j == 0)
        def _():
            top_s[...] = jnp.full_like(top_s, NEG)
            mix_s[...] = jnp.zeros_like(mix_s)

        @pl.when(j < per * iq)
        def _():
            block(iq, j, False)

        @pl.when(j >= per * iq)
        def _():
            block(iq, j, True)

        @pl.when(j == per * (iq + 1) - 1)
        def _():
            rows = pl.ds(pl.multiple_of(iq * bq, bq), bq)
            for i in range(heads):
                top, weight = top_s[i : i + 1, :], mix_s[i, HEAD : HEAD + 1, :]
                out[_head(i), rows] = (mix_s[i, :HEAD, :] * (1 / weight)).astype(LOW)
                lse[i : i + 1, rows] = top * scale + jnp.log(weight)

    def work(n, c):
        if c == 0:
            @pl.when(n > 0)
            def _():
                p, g = (n - 1) // CHIPS, (n - 1) % CHIPS
                for way in range(2):
                    for i in range(2):
                        swap(p, g, way, i, 1 - core).wait_recv()
                for copy in fetch(n - 1):
                    copy.start()

            @pl.when((n > 1) & (n < CHIPS + 2))
            def _():
                turn_over(n - 2)
        else:
            @pl.when(n > 0)
            def _():
                for copy in fetch(n - 1):
                    copy.wait()

            @pl.when((n > 0) & (n <= CHIPS))
            def _():
                project(n - 1)

            @pl.when(n > CHIPS)
            def _():
                products(n - 1)

        @pl.when(n > CHIPS)
        def _():
            first = (2 * (n - CHIPS - 1) + c) * total // (2 * CHIPS - 2)
            lax.fori_loop(first, (2 * (n - CHIPS - 1) + c + 1) * total // (2 * CHIPS - 2), lambda m, _: attend(m), None)

    def step(n, _):
        p, g = n // CHIPS, n % CHIPS
        for c in range(2):
            @pl.when(g > 0)
            def _():
                for way in range(2):
                    arrival(p, g, way, c).wait_recv()

            @pl.when(g < CHIPS - 1)
            def _():
                for way in range(2):
                    hop(p, g, way, c).start()

            for way in range(2):
                swap(p, g, way, c, core).start()
            work(n, c)

    steps = 2 * CHIPS
    lax.fori_loop(0, steps, step, None)
    results = [pltpu.make_async_copy(a, b, result_sem.at[n])
               for n, (a, b) in enumerate(((q, q_h), (k, k_h), (v, v_h), (out, out_h), (lse, lse_h), (by, by_h)))]
    for copy in results[:-1]:
        copy.start()
    for way in range(2):
        for i in range(2):
            swap(1, CHIPS - 1, way, i, 1 - core).wait_recv()
    for copy in fetch(steps - 1):
        copy.start()
    for copy in fetch(steps - 1):
        copy.wait()
    products(steps - 1)
    results[-1].start()

    def sent(n, _):
        p, g = n // CHIPS, n % CHIPS
        for way in range(2):
            for c in range(2):
                swap(p, g, way, c, core).wait_send()

                @pl.when(g < CHIPS - 1)
                def _():
                    hop(p, g, way, c).wait_send()

    lax.fori_loop(0, steps, sent, None)
    for copy in put(CHIPS - 1):
        copy.wait()
    for copy in results:
        copy.wait()


def gather(x, dy, gain, wq, wk, wv, wo, far, near):
    width, rows = x.shape[1], GROUP * ROWS
    heads = ROWS // HEAD
    vmem, dma = pltpu.VMEM, pltpu.SemaphoreType.DMA
    here = pl.BlockSpec(memory_space=pltpu.VMEM)
    by_token, by_head, log = (rows, ROWS), (ROWS, rows), (heads, rows)
    shapes = [((2, rows, width), LOW), ((width, rows), LOW), *[(by_token, LOW)] * 4, (by_head, LOW), (log, F32)]
    return pl.pallas_call(
        _gather,
        in_specs=[ANY, ANY, here, ANY, ANY, ANY, ANY, here, here],
        out_specs=[ANY] * 8,
        out_shape=[jax.ShapeDtypeStruct(*shape) for shape in shapes],
        scratch_shapes=[
            vmem(x.shape, LOW), vmem(x.shape, LOW), vmem((width, 3 * ROWS), LOW), vmem((ROWS, width), LOW), vmem((2, SPAN, width), LOW),
            vmem((width, SPAN), LOW), *[vmem(by_token, LOW)] * 4, vmem(by_head, LOW), vmem(log, F32),
            vmem((heads, QUERIES), F32), vmem((heads, HEAD + 8, QUERIES), F32), vmem((KEYS, QUERIES), jnp.int32),
            dma((6,)), dma((2,)), *[dma((2, CHIPS, 2, 2))] * 4, dma((2, 4)), dma((4,)), dma((6,)),
        ],
        compiler_params=pltpu.CompilerParams(collective_id=1, has_side_effects=True, vmem_limit_bytes=VMEM),
        cost_estimate=pl.CostEstimate(flops=2 * rows * width * ROWS * 6, transcendentals=rows * rows, bytes_accessed=rows * width * 8),
    )(x, dy, gain, wq, wk, wv, wo, far, near)

def solution(mesh):
    def step(x, dy, gain, wq, wk, wv, wo):
        gain = gain[None]
        far, near = tables(GROUP * ROWS)
        gathered, at, q, k, v, by_seen, out, lse = gather(x, dy, gain, wq, wk, wv, wo, far, near)
        dq, dk, dv = attend_bwd(q, k, v, by_seen, out, lse, far, near)
        return tuple(scatter(dq, dk, dv, wq, wk, wv, at, gathered, out, x, dy, gain))

    tokens, columns = P(("dp", "tp"), None), P(None, "tp")
    return jax.shard_map(
        step,
        mesh=mesh,
        in_specs=(tokens, tokens, P(None), columns, columns, columns, P("tp", None)),
        out_specs=(tokens, P("dp", None), P("dp", "tp"), P("dp", "tp"), P("dp", "tp"), P(("dp", "tp"), None)),
        check_vma=False,
    )
```

```python
import functools

import jax
import jax.numpy as jnp
import numpy as np
from jax import lax
from jax.experimental import pallas as pl
from jax.experimental.pallas import tpu as pltpu
from jax.sharding import PartitionSpec as P

NEG = -1e30
HIDDEN = 2 * NEG
LOG2E = 1.4426950408889634
VMEM = 62 * 2**20
STRIP = 512
KEYS = 512
HEAD = 128
THETA = 10000
ANGLES = 128
EPS = 1e-6
MESH = pl.DeviceIdType.MESH
ANY = pl.BlockSpec(memory_space=pl.ANY)
LOW = jnp.bfloat16
F32 = jnp.float32


def _dot(a, b, ca, cb):
    return lax.dot_general(a, b, (((ca,), (cb,)), ((), ())), preferred_element_type=F32)


def _gap(bk, bq):
    return lax.broadcasted_iota(jnp.int32, (bk, bq), 1) - lax.broadcasted_iota(jnp.int32, (bk, bq), 0)


def _head(i):
    return slice(i * HEAD, (i + 1) * HEAD)


def _pieces(heads, bq):
    return [(i, slice(at, at + STRIP)) for i in range(heads) for at in range(0, bq, STRIP)]


def _angle(m, far, near):
    here = pl.ds(m, 1)
    cos = far[0, here, :] * near[0] - far[1, here, :] * near[1]
    sin = far[1, here, :] * near[0] + far[0, here, :] * near[1]
    return cos, jnp.where(lax.broadcasted_iota(jnp.int32, sin.shape, 1) < HEAD // 2, sin, -sin)


def _turn(t, angle, way):
    cos, sin = angle
    t = t.astype(LOW).astype(F32)
    swapped = pltpu.roll(t, HEAD // 2, 1) * sin
    return (t * cos + (swapped if way else -swapped)).astype(LOW)


GROUP = 16
CHIPS = GROUP // 2
ROWS = 256
STEP = ROWS // 4
BAND = 16


def _ring_chip(place):
    return jnp.where(place < CHIPS // 2, place, CHIPS + CHIPS // 2 - 1 - place)


def _greet(others):
    barrier = pltpu.get_barrier_semaphore()
    for other in others:
        pl.semaphore_signal(barrier, inc=1, device_id={"tp": other}, device_id_type=MESH)
    pl.semaphore_wait(barrier, len(others))


def _scatter(dq_h, dk_h, dv_h, wq_h, wk_h, wv_h, at_h, dy_h, seen_h, x_h, my_dy_h, gain_h, dx_ref, dgain_ref, dwq_h, dwk_h, dwv_h, dwo_h,
             dqkv, w, seen, x_s, my_dy, gain, lhs, own, twin_out, twin_in, ring_out, ring_in, total_s, unit_sum, gain_out, gain_in,
             at_s, dy_s, dw_s, dwo_s,
             load_sem, twin_send, twin_recv, ring_send, ring_recv, gain_send, gain_recv, at_sem, dy_sem, dw_sem, dwo_sem):
    me = lax.axis_index("tp")
    chip, core = me // 2, me % 2
    place = _ring_chip(chip)
    twin = 2 * chip + 1 - core
    after = 2 * _ring_chip((place + 1) % CHIPS) + core
    before = 2 * _ring_chip((place + CHIPS - 1) % CHIPS) + core
    width = w.shape[0]
    part = [slice(n * ROWS, (n + 1) * ROWS) for n in range(3)]

    given = (*((a, dqkv.at[:, here]) for a, here in zip((dq_h, dk_h, dv_h), part)), *((a, w.at[:, here]) for a, here in zip((wq_h, wk_h, wv_h), part)),
             (seen_h, seen), (x_h, x_s), (my_dy_h, my_dy), (gain_h, gain))
    loads = [pltpu.make_async_copy(a, b, load_sem.at[n]) for n, (a, b) in enumerate(given)]
    for load in loads:
        load.start()

    def fetch(u, slot):
        here = pl.ds(pl.multiple_of(u * ROWS, ROWS), ROWS)
        return (pltpu.make_async_copy(at_h.at[here, :], at_s.at[slot], at_sem.at[slot]),
                pltpu.make_async_copy(dy_h.at[1, :, here], dy_s.at[slot], dy_sem.at[slot]))

    def put(u, slot):
        here = pl.ds(pl.multiple_of(u * ROWS, ROWS), ROWS)
        return (*(pltpu.make_async_copy(dw_s.at[slot, n], out.at[here, :], dw_sem.at[slot, n]) for n, out in enumerate((dwq_h, dwk_h, dwv_h))),
                pltpu.make_async_copy(dwo_s.at[slot], dwo_h.at[:, here], dwo_sem.at[slot]))

    for copy in fetch(0, 0):
        copy.start()
    others = [(me + d) % GROUP for d in range(1, GROUP)]
    _greet(others)

    def swap(slot, c):
        return pltpu.make_async_remote_copy(src_ref=twin_out.at[slot, c], dst_ref=twin_in.at[slot, c], send_sem=twin_send.at[slot, c],
                                            recv_sem=twin_recv.at[slot, c], device_id={"tp": twin}, device_id_type=MESH)

    def hop(slot, way, c):
        here = pl.ds(way * STEP, STEP)
        return pltpu.make_async_remote_copy(src_ref=ring_out.at[c, here, :], dst_ref=ring_in.at[slot, c, here, :], send_sem=ring_send.at[way, c],
                                            recv_sem=ring_recv.at[slot, way, c], device_id={"tp": before if way else after}, device_id_type=MESH)

    def terms(s, c):
        forth = _ring_chip((place + 2 * CHIPS - 1 - s) % CHIPS)
        back = _ring_chip((place + 1 + s) % CHIPS)
        starts = [(2 * to + of) * ROWS + (2 * way + c) * STEP for of in (core, 1 - core) for way, to in ((0, forth), (1, back))]
        for n, start in enumerate(starts):
            lhs[n * STEP : (n + 1) * STEP, :] = dqkv[pl.ds(pl.multiple_of(start, STEP), STEP), :]
        slot = s % 2

        def columns(j, _):
            here = pl.ds(pl.multiple_of(j * STRIP, STRIP), STRIP)
            term = _dot(lhs[...], w[here, :], 1, 1)
            own[c, :, here] = term[: 2 * STEP]
            twin_out[slot, c, :, here] = term[2 * STEP :].astype(LOW)

        lax.fori_loop(0, width // STRIP, columns, None)
        swap(slot, c).start()

    def add(s, c, ringed, last):
        slot = s % 2

        def columns(j, _):
            here = pl.ds(pl.multiple_of(j * ROWS, ROWS), ROWS)
            total = own[c, :, here] + twin_in[slot, c, :, here].astype(F32)
            if ringed:
                total += ring_in[1 - slot, c, :, here].astype(F32)
            if last:
                total_s[:, here] = total
            else:
                ring_out[c, :, here] = total.astype(LOW)

        lax.fori_loop(0, width // ROWS, columns, None)

    def norm(c):
        def band(j, _):
            src = pl.ds(pl.multiple_of(j * BAND, BAND), BAND)
            at = c * STEP + j * BAND + jnp.where(j >= STEP // BAND, STEP, 0)
            dst = pl.ds(pl.multiple_of(at, BAND), BAND)
            wide, by = x_s[dst, :].astype(F32), total_s[src, :]
            scale = lax.rsqrt(jnp.mean(wide * wide, -1, keepdims=True) + EPS)
            unit = wide * scale
            unit_sum[...] += by * unit
            by = by * gain[...].astype(F32)
            dx = scale * (by - unit * jnp.mean(by * unit, -1, keepdims=True))
            dx_ref[dst, :] = (my_dy[dst, :].astype(F32) + dx).astype(LOW)

        lax.fori_loop(0, 2 * STEP // BAND, band, None)

    def weights(u, slot):
        for copy in fetch(u, slot):
            copy.wait()

        @pl.when(u < GROUP - 1)
        def _():
            for copy in fetch(u + 1, 1 - slot):
                copy.start()

        @pl.when(u >= 2)
        def _():
            for copy in put(u, slot):
                copy.wait()

        for n in range(3):
            dw_s[slot, n] = _dot(at_s[slot], dqkv[:, part[n]], 1, 0).astype(LOW)
        dwo_s[slot] = _dot(seen[...], dy_s[slot], 1, 0).astype(LOW)
        for copy in put(u, slot):
            copy.start()

    for load in loads[:6]:
        load.wait()
    for c in range(2):
        terms(0, c)
    for load in loads[6:]:
        load.wait()
    unit_sum[...] = jnp.zeros_like(unit_sum)
    last = CHIPS - 1

    def step(s, _):
        slot = s % 2
        for c in range(2):
            swap(slot, c).wait_recv()

            @pl.when(s == 0)
            def _():
                add(s, c, False, False)

            @pl.when(s > 0)
            def _():
                for way in range(2):
                    hop(1 - slot, way, c).wait()
                add(s, c, True, False)

            for way in range(2):
                hop(slot, way, c).start()

            @pl.when(s > 0)
            def _():
                swap(1 - slot, c).wait_send()

            terms(s + 1, c)
            weights(2 * s + c, c)

    lax.fori_loop(0, last, step, None)
    for c in range(2):
        swap(last % 2, c).wait_recv()
        for way in range(2):
            hop(1 - last % 2, way, c).wait()
        add(last, c, True, True)
        norm(c)
        if c == 0:
            weights(2 * last, c)
    gain_out[...] = unit_sum[...].sum(0, keepdims=True)
    gain_in[me] = gain_out[...]
    copies = [pltpu.make_async_remote_copy(src_ref=gain_out, dst_ref=gain_in.at[me], send_sem=gain_send.at[n], recv_sem=gain_recv.at[n],
                                           device_id={"tp": other}, device_id_type=MESH) for n, other in enumerate(others)]
    for copy in copies:
        copy.start()
    weights(2 * last + 1, 1)
    for copy in copies:
        copy.wait()
    dgain_ref[...] = functools.reduce(lambda a, b: a + b, [gain_in[n] for n in range(GROUP)])
    for c in range(2):
        for slot in range(2):
            swap(slot, c).wait_send()
        for copy in put(2 * last + c, c):
            copy.wait()


def scatter(dq, dk, dv, wq, wk, wv, at, dy, seen, x, my_dy, gain):
    width, rows = at.shape
    vmem, dma = pltpu.VMEM, pltpu.SemaphoreType.DMA
    here = pl.BlockSpec(memory_space=pltpu.VMEM)
    part, mine = 2 * STEP, (ROWS, width)
    by_weight = jax.ShapeDtypeStruct((width, ROWS), LOW)
    return pl.pallas_call(
        _scatter,
        in_specs=[ANY] * 12,
        out_specs=[here] * 2 + [ANY] * 4,
        out_shape=[jax.ShapeDtypeStruct(mine, LOW), jax.ShapeDtypeStruct((1, width), F32)] + [by_weight] * 3 + [jax.ShapeDtypeStruct(mine, LOW)],
        scratch_shapes=[
            vmem((rows, 3 * ROWS), LOW), vmem((width, 3 * ROWS), LOW), vmem(seen.shape, LOW), vmem(mine, LOW), vmem(mine, LOW), vmem((1, width), LOW),
            vmem((4 * STEP, 3 * ROWS), LOW),
            vmem((2, part, width), F32), vmem((2, 2, part, width), LOW), vmem((2, 2, part, width), LOW),
            vmem((2, part, width), LOW), vmem((2, 2, part, width), LOW), vmem((part, width), F32), vmem((BAND, width), F32),
            vmem((1, width), F32), vmem((GROUP, 1, width), F32),
            vmem((2, ROWS, rows), LOW), vmem((2, rows, ROWS), LOW), vmem((2, 3, ROWS, ROWS), LOW), vmem((2, ROWS, ROWS), LOW),
            dma((10,)), dma((2, 2)), dma((2, 2)), dma((2, 2)), dma((2, 2, 2)), dma((GROUP - 1,)), dma((GROUP - 1,)),
            dma((2,)), dma((2,)), dma((2, 3)), dma((2,)),
        ],
        compiler_params=pltpu.CompilerParams(collective_id=0, has_side_effects=True, vmem_limit_bytes=VMEM),
        cost_estimate=pl.CostEstimate(flops=2 * rows * width * ROWS * 7, transcendentals=0, bytes_accessed=rows * width * 6),
    )(dq, dk, dv, wq, wk, wv, at, dy, seen, x, my_dy, gain)


def tables(rows):
    half = HEAD // 2
    rate = float(THETA) ** (-(np.arange(HEAD) % half) / half)
    turns = [np.arange(0, rows, ANGLES)[:, None] * rate, np.arange(ANGLES)[:, None] * rate]
    return [jnp.asarray(np.stack([np.cos(t), np.sin(t)]), F32) for t in turns]


HALF = ROWS // 2
SPAN = 4 * HALF
QUERIES = 1024


def _gather(x_h, dy_h, gain, wq_h, wk_h, wv_h, wo_h, far, near, all_h, at_h, dq_h, dk_h, dv_h, out_h,
            x_s, mine, w, wo, lhs, turned_s, q, k, v, by, out, lse, top_s, mix_s, gap_s, asked_s, facts_s, dq_s, dk_s, dv_s, lag_s,
            load_sem, store_sem, hop_send, hop_recv, swap_send, swap_recv, lhs_sem, at_sem, result_sem):
    me = lax.axis_index("tp")
    chip, core = me // 2, me % 2
    place = _ring_chip(chip)
    twin = 2 * chip + 1 - core
    ways = [2 * _ring_chip((place + d) % CHIPS) + core for d in (1, CHIPS - 1)]
    barrier = pltpu.get_barrier_semaphore()
    for other in (twin, *ways):
        pl.semaphore_signal(barrier, inc=1, device_id={"tp": other}, device_id_type=MESH)
    part = [slice(n * ROWS, (n + 1) * ROWS) for n in range(3)]
    width = x_s.shape[1]
    heads, bq, bk, scale = ROWS // HEAD, QUERIES, KEYS, HEAD**-0.5
    e = scale * LOG2E

    given = ((x_h, x_s), (dy_h, lhs.at[0, :ROWS, :]), *((a, w.at[:, here]) for a, here in zip((wq_h, wk_h, wv_h), part)), (wo_h, wo))
    loads = [pltpu.make_async_copy(a, b, load_sem.at[n]) for n, (a, b) in enumerate(given)]
    for load in loads:
        load.start()
    here = pl.ds(pl.multiple_of(me * ROWS, ROWS), ROWS)
    stores = [pltpu.make_async_copy(a, all_h.at[n, here, :], store_sem.at[n]) for n, a in enumerate((mine, lhs.at[0, :ROWS, :]))]
    loads[0].wait()

    def norm(j, _):
        band = pl.ds(pl.multiple_of(j * BAND, BAND), BAND)
        wide = x_s[band, :].astype(F32)
        mine[band, :] = (wide * lax.rsqrt(jnp.mean(wide * wide, -1, keepdims=True) + EPS) * gain[...].astype(F32)).astype(LOW)

    lax.fori_loop(0, ROWS // BAND, norm, None)
    stores[0].start()
    loads[1].wait()
    stores[1].start()
    gap_s[...] = _gap(bk, bq)
    column = lax.broadcasted_iota(jnp.int32, lag_s.shape, 1)
    lag_s[...] = column + jnp.where(column >= HALF, HALF, 0) - lax.broadcasted_iota(jnp.int32, lag_s.shape, 0)
    dk_s[...] = jnp.zeros_like(dk_s)
    dv_s[...] = jnp.zeros_like(dv_s)
    for store in stores:
        store.wait()
    for load in loads[2:]:
        load.wait()
    pl.semaphore_wait(barrier, 3)

    def begins(way, g):
        return _ring_chip((place + (g if way else 2 * CHIPS - g)) % CHIPS)

    def piece(p, g, way, c, of):
        start = (2 * begins(way, g) + of) * ROWS + way * HALF + c * STEP
        return all_h.at[p, pl.ds(pl.multiple_of(start, STEP), STEP), :]

    def hop(p, g, way, c):
        rows = piece(p, g, way, c, core)
        return pltpu.make_async_remote_copy(src_ref=rows, dst_ref=rows, send_sem=hop_send.at[p, g, way, c], recv_sem=hop_recv.at[p, g, way, c],
                                            device_id={"tp": ways[way]}, device_id_type=MESH)

    def arrival(p, g, way, c):
        rows = piece(p, g, way, c, core)
        return pltpu.make_async_remote_copy(src_ref=rows, dst_ref=rows, send_sem=hop_send.at[p, g - 1, way, c],
                                            recv_sem=hop_recv.at[p, g - 1, way, c], device_id={"tp": ways[way]}, device_id_type=MESH)

    def swap(p, g, way, c, of):
        rows = piece(p, g, way, c, of)
        return pltpu.make_async_remote_copy(src_ref=rows, dst_ref=rows, send_sem=swap_send.at[p, g, way, c], recv_sem=swap_recv.at[p, g, way, c],
                                            device_id={"tp": twin}, device_id_type=MESH)

    def starts(g):
        return [(2 * begins(way, g) + of) * ROWS + way * HALF for way in range(2) for of in range(2)]

    def fetch(n):
        return [pltpu.make_async_copy(all_h.at[n // CHIPS, pl.ds(pl.multiple_of(start, HALF), HALF), :],
                                      lhs.at[n % 2, i * HALF : (i + 1) * HALF, :], lhs_sem.at[n % 2, i]) for i, start in enumerate(starts(n % CHIPS))]

    def put(g):
        return [pltpu.make_async_copy(turned_s.at[:, i * HALF : (i + 1) * HALF], at_h.at[:, pl.ds(pl.multiple_of(start, HALF), HALF)], at_sem.at[i])
                for i, start in enumerate(starts(g))]

    def project(n):
        begin = starts(n % CHIPS)
        for m, to in enumerate((q, k, v)):
            got = _dot(lhs[n % 2], w[:, part[m]], 1, 0).astype(LOW)
            for i, start in enumerate(begin):
                rows = pl.ds(pl.multiple_of(start, HALF), HALF)
                angle = _angle(start // ANGLES, far, near)
                for h in range(heads):
                    t = got[i * HALF : (i + 1) * HALF, _head(h)]
                    to[rows, _head(h)] = t if m == 2 else _turn(t, angle, 0)

    def turn_over(n):
        @pl.when(n > 0)
        def _():
            for copy in put(n - 1):
                copy.wait()

        def columns(j, _):
            here = pl.ds(pl.multiple_of(j * STRIP, STRIP), STRIP)
            turned_s[here, :] = lhs[n % 2, :, here].T

        lax.fori_loop(0, width // STRIP, columns, None)
        for copy in put(n):
            copy.start()

    def products(n):
        by[n % CHIPS] = _dot(lhs[n % 2], wo[...], 1, 1).astype(LOW)

    def block(iq, j, masked):
        ones = jnp.ones((8, bk), LOW)
        keys = pl.ds(pl.multiple_of(j * bk, bk), bk)
        pieces = _pieces(heads, bq)
        asked = [pl.ds(pl.multiple_of(iq * bq + at.start, STRIP), STRIP) for _, at in pieces]
        scores = [_dot(k[keys, _head(i)], q[rows, _head(i)], 1, 1) for (i, _), rows in zip(pieces, asked)]
        ok = gap_s[...] >= j * bk - iq * bq if masked else None
        weights, keeps = [], []
        for (i, at), s in zip(pieces, scores):
            if masked:
                s = jnp.where(ok[:, at], s, HIDDEN)
            old = top_s[i : i + 1, at]
            top = jnp.maximum(old, s.max(axis=0, keepdims=True))
            top_s[i : i + 1, at] = top
            weights.append(jnp.exp2((s - top) * e).astype(LOW))
            keeps.append(jnp.exp2((old - top) * e))
        for (i, at), p, keep in zip(pieces, weights, keeps):
            values = jnp.concatenate([v[keys, _head(i)].T, ones], axis=0)
            mix_s[i, :, at] = mix_s[i, :, at] * keep + _dot(values, p, 1, 0)

    per = bq // bk
    count = width // bq
    total = per * count * (count + 1) // 2

    def attend(n):
        iq = sum((n >= per * i * (i + 1) // 2).astype(jnp.int32) for i in range(1, count))
        j = n - per * iq * (iq + 1) // 2

        @pl.when(j == 0)
        def _():
            top_s[...] = jnp.full_like(top_s, NEG)
            mix_s[...] = jnp.zeros_like(mix_s)

        @pl.when(j < per * iq)
        def _():
            block(iq, j, False)

        @pl.when(j >= per * iq)
        def _():
            block(iq, j, True)

        @pl.when(j == per * (iq + 1) - 1)
        def _():
            rows = pl.ds(pl.multiple_of(iq * bq, bq), bq)
            for i in range(heads):
                top, weight = top_s[i : i + 1, :], mix_s[i, HEAD : HEAD + 1, :]
                out[_head(i), rows] = (mix_s[i, :HEAD, :] * (1 / weight)).astype(LOW)
                lse[i : i + 1, rows] = top * scale + jnp.log(weight)

    def back(ways, g, j, masked):
        keys = pl.ds(pl.multiple_of(j * bk, bk), bk)
        pieces = [(way, i) for way in ways for i in range(heads)]
        qs = [asked_s[way, :, _head(i)] for way, i in pieces]
        dos = [by[g, pl.ds(pl.multiple_of(way * ROWS, ROWS), ROWS), _head(i)] for way, i in pieces]
        scores = [_dot(k[keys, _head(i)], x, 1, 1) for (_, i), x in zip(pieces, qs)]
        dps = [_dot(v[keys, _head(i)], x, 1, 1) for (_, i), x in zip(pieces, dos)]
        for n, (way, i) in enumerate(pieces):
            p = jnp.exp2(scores[n] * e - facts_s[way, i : i + 1, :])
            if masked:
                p = jnp.where(lag_s[...] >= -HALF * way, p, 0.0)
            ds = (p * (dps[n] - facts_s[way, heads + i : heads + i + 1, :])).astype(LOW)
            dv_s[i, keys, :] += _dot(p.astype(LOW), dos[n], 1, 0)
            dk_s[i, keys, :] += _dot(ds, qs[n], 1, 0)
            dq_s[way, i] += _dot(k[keys, _head(i)].T, ds, 1, 0)

    def backward(g):
        begin = starts(g)
        dq_s[...] = jnp.zeros_like(dq_s)
        for n, start in enumerate(begin):
            rows, way = pl.ds(pl.multiple_of(start, HALF), HALF), n // 2
            at = slice(n % 2 * HALF, (n % 2 + 1) * HALF)
            asked_s[way, at, :] = q[rows, :]
            for i in range(heads):
                facts_s[way, i : i + 1, at] = lse[i : i + 1, rows] * LOG2E
                d_out = by[g, n * HALF : (n + 1) * HALF, _head(i)].astype(F32).T
                facts_s[way, heads + i : heads + i + 1, at] = (d_out * out[_head(i), rows].astype(F32)).sum(0, keepdims=True)
        ends = [begins(way, g) for way in range(2)]
        least, most = jnp.minimum(*ends), jnp.maximum(*ends)
        late = (ends[1] > ends[0]).astype(jnp.int32)
        lax.fori_loop(0, least, lambda j, _: back((0, 1), g, j, False), None)
        lax.fori_loop(least, most, lambda j, _: back((late,), g, j, False), None)
        lax.fori_loop(0, 2, lambda way, _: back((way,), g, jnp.where(way == late, most, least), True), None)
        for n, start in enumerate(begin):
            rows, way = pl.ds(pl.multiple_of(start, HALF), HALF), n // 2
            angle = _angle(start // ANGLES, far, near)
            for i in range(heads):
                q[rows, _head(i)] = _turn((dq_s[way, i, :, n % 2 * HALF : (n % 2 + 1) * HALF] * scale).T, angle, 1)

    steps = 2 * CHIPS
    first, share = steps + 1, 4
    began = first + total // share

    def work(m, n, c):
        @pl.when((c == 0) & (n > 0))
        def _():
            for copy in fetch(n - 1):
                copy.wait()

            @pl.when(n <= CHIPS)
            def _():
                project(n - 1)

            @pl.when(n > CHIPS)
            def _():
                products(n - 1)

        @pl.when((c == 1) & (n > 0) & (n <= CHIPS))
        def _():
            turn_over(n - 1)

        @pl.when((m >= first) & (m < began))
        def _():
            lax.fori_loop(share * (m - first), share * (m - first + 1), lambda i, _: attend(i), None)

        @pl.when((m >= began) & ((m <= began + share) | (c == 0)))
        def _():
            backward(jnp.where(m <= began + share, m - began, n - CHIPS - 1))

        @pl.when((c == 1) & (n < steps))
        def _():
            for way in range(2):
                for i in range(2):
                    swap(n // CHIPS, n % CHIPS, way, i, 1 - core).wait_recv()
            for copy in fetch(n):
                copy.start()

    def step(m, _):
        n, c = m // 2, m % 2
        p, g = n // CHIPS, n % CHIPS

        @pl.when((g > 0) & (n < steps))
        def _():
            for way in range(2):
                arrival(p, g, way, c).wait_recv()

        @pl.when((g < CHIPS - 1) & (n < steps))
        def _():
            for way in range(2):
                hop(p, g, way, c).start()

        @pl.when(n < steps)
        def _():
            for way in range(2):
                swap(p, g, way, c, core).start()

        work(m, n, c)

    lax.fori_loop(0, 2 * steps + 1, step, None)

    def finish(j, _):
        here = pl.ds(pl.multiple_of(j * ANGLES, ANGLES), ANGLES)
        angle = _angle(j, far, near)
        for i in range(heads):
            k[here, _head(i)] = _turn(dk_s[i, here, :] * scale, angle, 1)
            v[here, _head(i)] = dv_s[i, here, :].astype(LOW)

    results = [pltpu.make_async_copy(a, b, result_sem.at[n]) for n, (a, b) in enumerate(((out, out_h), (q, dq_h), (k, dk_h), (v, dv_h)))]
    for copy in results[:2]:
        copy.start()
    lax.fori_loop(0, width // ANGLES, finish, None)
    for copy in results[2:]:
        copy.start()

    def sent(n, _):
        p, g = n // CHIPS, n % CHIPS
        for way in range(2):
            for c in range(2):
                swap(p, g, way, c, core).wait_send()

                @pl.when(g < CHIPS - 1)
                def _():
                    hop(p, g, way, c).wait_send()

    lax.fori_loop(0, steps, sent, None)
    for copy in put(CHIPS - 1):
        copy.wait()
    for copy in results:
        copy.wait()


def gather(x, dy, gain, wq, wk, wv, wo, far, near):
    width, rows = x.shape[1], GROUP * ROWS
    heads = ROWS // HEAD
    vmem, dma = pltpu.VMEM, pltpu.SemaphoreType.DMA
    here = pl.BlockSpec(memory_space=pltpu.VMEM)
    by_token, by_head, sums = (rows, ROWS), (ROWS, rows), (heads, rows, HEAD)
    shapes = [(2, rows, width), (width, rows), by_token, by_token, by_token, by_head]
    return pl.pallas_call(
        _gather,
        in_specs=[ANY, ANY, here, ANY, ANY, ANY, ANY, here, here],
        out_specs=[ANY] * len(shapes),
        out_shape=[jax.ShapeDtypeStruct(shape, LOW) for shape in shapes],
        scratch_shapes=[
            vmem(x.shape, LOW), vmem(x.shape, LOW), vmem((width, 3 * ROWS), LOW), vmem((ROWS, width), LOW), vmem((2, SPAN, width), LOW),
            vmem((width, SPAN), LOW), *[vmem(by_token, LOW)] * 3, vmem((CHIPS, SPAN, ROWS), LOW), vmem(by_head, LOW), vmem((heads, rows), F32),
            vmem((heads, QUERIES), F32), vmem((heads, HEAD + 8, QUERIES), F32), vmem((KEYS, QUERIES), jnp.int32),
            vmem((2, ROWS, ROWS), LOW), vmem((2, 2 * heads, ROWS), F32), vmem((2, heads, HEAD, ROWS), F32), vmem(sums, F32), vmem(sums, F32),
            vmem((KEYS, ROWS), jnp.int32),
            dma((6,)), dma((2,)), *[dma((2, CHIPS, 2, 2))] * 4, dma((2, 4)), dma((4,)), dma((4,)),
        ],
        compiler_params=pltpu.CompilerParams(collective_id=1, has_side_effects=True, vmem_limit_bytes=VMEM),
        cost_estimate=pl.CostEstimate(flops=2 * rows * width * ROWS * 8, transcendentals=rows * rows, bytes_accessed=rows * width * 8),
    )(x, dy, gain, wq, wk, wv, wo, far, near)

def solution(mesh):
    def step(x, dy, gain, wq, wk, wv, wo):
        gain = gain[None]
        far, near = tables(GROUP * ROWS)
        gathered, at, dq, dk, dv, out = gather(x, dy, gain, wq, wk, wv, wo, far, near)
        return tuple(scatter(dq, dk, dv, wq, wk, wv, at, gathered, out, x, dy, gain))

    tokens, columns = P(("dp", "tp"), None), P(None, "tp")
    return jax.shard_map(
        step,
        mesh=mesh,
        in_specs=(tokens, tokens, P(None), columns, columns, columns, P("tp", None)),
        out_specs=(tokens, P("dp", None), P("dp", "tp"), P("dp", "tp"), P("dp", "tp"), P(("dp", "tp"), None)),
        check_vma=False,
    )
```

```python
import functools

import jax
import jax.numpy as jnp
import numpy as np
from jax import lax
from jax.experimental import pallas as pl
from jax.experimental.pallas import tpu as pltpu
from jax.sharding import PartitionSpec as P

NEG = -1e30
HIDDEN = 2 * NEG
LOG2E = 1.4426950408889634
VMEM = 62 * 2**20
STRIP = 512
KEYS = 512
HEAD = 128
THETA = 10000
ANGLES = 128
EPS = 1e-6
MESH = pl.DeviceIdType.MESH
ANY = pl.BlockSpec(memory_space=pl.ANY)
LOW = jnp.bfloat16
F32 = jnp.float32


def _dot(a, b, ca, cb):
    return lax.dot_general(a, b, (((ca,), (cb,)), ((), ())), preferred_element_type=F32)


def _gap(bk, bq):
    return lax.broadcasted_iota(jnp.int32, (bk, bq), 1) - lax.broadcasted_iota(jnp.int32, (bk, bq), 0)


def _head(i):
    return slice(i * HEAD, (i + 1) * HEAD)


def _pieces(heads, bq):
    return [(i, slice(at, at + STRIP)) for i in range(heads) for at in range(0, bq, STRIP)]


def _angle(m, far, near):
    here = pl.ds(m, 1)
    cos = far[0, here, :] * near[0] - far[1, here, :] * near[1]
    sin = far[1, here, :] * near[0] + far[0, here, :] * near[1]
    return cos, jnp.where(lax.broadcasted_iota(jnp.int32, sin.shape, 1) < HEAD // 2, sin, -sin)


def _turn(t, angle, way):
    cos, sin = angle
    t = t.astype(LOW).astype(F32)
    swapped = pltpu.roll(t, HEAD // 2, 1) * sin
    return (t * cos + (swapped if way else -swapped)).astype(LOW)


GROUP = 16
CHIPS = GROUP // 2
ROWS = 256
STEP = ROWS // 4
BAND = 16


def _ring_chip(place):
    return jnp.where(place < CHIPS // 2, place, CHIPS + CHIPS // 2 - 1 - place)


def _greet(others):
    barrier = pltpu.get_barrier_semaphore()
    for other in others:
        pl.semaphore_signal(barrier, inc=1, device_id={"tp": other}, device_id_type=MESH)
    pl.semaphore_wait(barrier, len(others))


def _scatter(dq_h, dk_h, dv_h, wq_h, wk_h, wv_h, at_h, dy_h, seen_h, x_h, my_dy_h, gain_h, dx_ref, dgain_ref, dwq_h, dwk_h, dwv_h, dwo_h,
             dqkv, w, seen, x_s, my_dy, gain, lhs, own, twin_out, twin_in, ring_out, ring_in, total_s, unit_sum, gain_out, gain_in,
             at_s, dy_s, dw_s, dwo_s,
             load_sem, twin_send, twin_recv, ring_send, ring_recv, gain_send, gain_recv, at_sem, dy_sem, dw_sem, dwo_sem):
    me = lax.axis_index("tp")
    chip, core = me // 2, me % 2
    place = _ring_chip(chip)
    twin = 2 * chip + 1 - core
    after = 2 * _ring_chip((place + 1) % CHIPS) + core
    before = 2 * _ring_chip((place + CHIPS - 1) % CHIPS) + core
    width = w.shape[0]
    part = [slice(n * ROWS, (n + 1) * ROWS) for n in range(3)]

    given = (*((a, dqkv.at[:, here]) for a, here in zip((dq_h, dk_h, dv_h), part)), *((a, w.at[:, here]) for a, here in zip((wq_h, wk_h, wv_h), part)),
             (seen_h, seen), (x_h, x_s), (my_dy_h, my_dy), (gain_h, gain))
    loads = [pltpu.make_async_copy(a, b, load_sem.at[n]) for n, (a, b) in enumerate(given)]
    for load in loads[:6]:
        load.start()

    def fetch(u, slot):
        here = pl.ds(pl.multiple_of(u * ROWS, ROWS), ROWS)
        return (pltpu.make_async_copy(at_h.at[here, :], at_s.at[slot], at_sem.at[slot]),
                pltpu.make_async_copy(dy_h.at[1, :, here], dy_s.at[slot], dy_sem.at[slot]))

    def put(u, slot):
        here = pl.ds(pl.multiple_of(u * ROWS, ROWS), ROWS)
        return (*(pltpu.make_async_copy(dw_s.at[slot, n], out.at[here, :], dw_sem.at[slot, n]) for n, out in enumerate((dwq_h, dwk_h, dwv_h))),
                pltpu.make_async_copy(dwo_s.at[slot], dwo_h.at[:, here], dwo_sem.at[slot]))

    others = [(me + d) % GROUP for d in range(1, GROUP)]
    _greet(others)

    def swap(slot, c):
        return pltpu.make_async_remote_copy(src_ref=twin_out.at[slot, c], dst_ref=twin_in.at[slot, c], send_sem=twin_send.at[slot, c],
                                            recv_sem=twin_recv.at[slot, c], device_id={"tp": twin}, device_id_type=MESH)

    def hop(slot, way, c):
        here = pl.ds(way * STEP, STEP)
        return pltpu.make_async_remote_copy(src_ref=ring_out.at[c, here, :], dst_ref=ring_in.at[slot, c, here, :], send_sem=ring_send.at[way, c],
                                            recv_sem=ring_recv.at[slot, way, c], device_id={"tp": before if way else after}, device_id_type=MESH)

    def terms(s, c):
        forth = _ring_chip((place + 2 * CHIPS - 1 - s) % CHIPS)
        back = _ring_chip((place + 1 + s) % CHIPS)
        starts = [(2 * to + of) * ROWS + (2 * way + c) * STEP for of in (core, 1 - core) for way, to in ((0, forth), (1, back))]
        for n, start in enumerate(starts):
            lhs[n * STEP : (n + 1) * STEP, :] = dqkv[pl.ds(pl.multiple_of(start, STEP), STEP), :]
        slot = s % 2

        def columns(j, _):
            here = pl.ds(pl.multiple_of(j * STRIP, STRIP), STRIP)
            term = _dot(lhs[...], w[here, :], 1, 1)
            own[c, :, here] = term[: 2 * STEP]
            twin_out[slot, c, :, here] = term[2 * STEP :].astype(LOW)

        lax.fori_loop(0, width // STRIP, columns, None)
        swap(slot, c).start()

    def add(s, c, ringed, last):
        slot = s % 2

        def columns(j, _):
            here = pl.ds(pl.multiple_of(j * ROWS, ROWS), ROWS)
            total = own[c, :, here] + twin_in[slot, c, :, here].astype(F32)
            if ringed:
                total += ring_in[1 - slot, c, :, here].astype(F32)
            if last:
                total_s[:, here] = total
            else:
                ring_out[c, :, here] = total.astype(LOW)

        lax.fori_loop(0, width // ROWS, columns, None)

    def norm(c):
        def band(j, _):
            src = pl.ds(pl.multiple_of(j * BAND, BAND), BAND)
            at = c * STEP + j * BAND + jnp.where(j >= STEP // BAND, STEP, 0)
            dst = pl.ds(pl.multiple_of(at, BAND), BAND)
            wide, by = x_s[dst, :].astype(F32), total_s[src, :]
            scale = lax.rsqrt(jnp.mean(wide * wide, -1, keepdims=True) + EPS)
            unit = wide * scale
            unit_sum[...] += by * unit
            by = by * gain[...].astype(F32)
            dx = scale * (by - unit * jnp.mean(by * unit, -1, keepdims=True))
            dx_ref[dst, :] = (my_dy[dst, :].astype(F32) + dx).astype(LOW)

        lax.fori_loop(0, 2 * STEP // BAND, band, None)

    def weights(u, slot):
        for copy in fetch(u, slot):
            copy.wait()

        @pl.when(u < GROUP - 1)
        def _():
            for copy in fetch(u + 1, 1 - slot):
                copy.start()

        @pl.when(u >= 2)
        def _():
            for copy in put(u, slot):
                copy.wait()

        for n in range(3):
            dw_s[slot, n] = _dot(at_s[slot], dqkv[:, part[n]], 1, 0).astype(LOW)
        dwo_s[slot] = _dot(seen[...], dy_s[slot], 1, 0).astype(LOW)
        for copy in put(u, slot):
            copy.start()

    for load in loads[:6]:
        load.wait()
    for load in loads[6:]:
        load.start()
    for copy in fetch(0, 0):
        copy.start()
    for c in range(2):
        terms(0, c)
    for load in loads[6:]:
        load.wait()
    unit_sum[...] = jnp.zeros_like(unit_sum)
    last = CHIPS - 1

    def step(s, _):
        slot = s % 2
        for c in range(2):
            swap(slot, c).wait_recv()

            @pl.when(s == 0)
            def _():
                add(s, c, False, False)

            @pl.when(s > 0)
            def _():
                for way in range(2):
                    hop(1 - slot, way, c).wait()
                add(s, c, True, False)

            for way in range(2):
                hop(slot, way, c).start()

            @pl.when(s > 0)
            def _():
                swap(1 - slot, c).wait_send()

            terms(s + 1, c)
            weights(2 * s + c, c)

    lax.fori_loop(0, last, step, None)
    for c in range(2):
        swap(last % 2, c).wait_recv()
        for way in range(2):
            hop(1 - last % 2, way, c).wait()
        add(last, c, True, True)
        norm(c)
        if c == 0:
            weights(2 * last, c)
    gain_out[...] = unit_sum[...].sum(0, keepdims=True)
    gain_in[me] = gain_out[...]
    copies = [pltpu.make_async_remote_copy(src_ref=gain_out, dst_ref=gain_in.at[me], send_sem=gain_send.at[n], recv_sem=gain_recv.at[n],
                                           device_id={"tp": other}, device_id_type=MESH) for n, other in enumerate(others)]
    for copy in copies:
        copy.start()
    weights(2 * last + 1, 1)
    for copy in copies:
        copy.wait()
    dgain_ref[...] = functools.reduce(lambda a, b: a + b, [gain_in[n] for n in range(GROUP)])
    for c in range(2):
        for slot in range(2):
            swap(slot, c).wait_send()
        for copy in put(2 * last + c, c):
            copy.wait()


def scatter(dq, dk, dv, wq, wk, wv, at, dy, seen, x, my_dy, gain):
    width, rows = at.shape
    vmem, dma = pltpu.VMEM, pltpu.SemaphoreType.DMA
    here = pl.BlockSpec(memory_space=pltpu.VMEM)
    part, mine = 2 * STEP, (ROWS, width)
    by_weight = jax.ShapeDtypeStruct((width, ROWS), LOW)
    return pl.pallas_call(
        _scatter,
        in_specs=[ANY] * 12,
        out_specs=[here] * 2 + [ANY] * 4,
        out_shape=[jax.ShapeDtypeStruct(mine, LOW), jax.ShapeDtypeStruct((1, width), F32)] + [by_weight] * 3 + [jax.ShapeDtypeStruct(mine, LOW)],
        scratch_shapes=[
            vmem((rows, 3 * ROWS), LOW), vmem((width, 3 * ROWS), LOW), vmem(seen.shape, LOW), vmem(mine, LOW), vmem(mine, LOW), vmem((1, width), LOW),
            vmem((4 * STEP, 3 * ROWS), LOW),
            vmem((2, part, width), F32), vmem((2, 2, part, width), LOW), vmem((2, 2, part, width), LOW),
            vmem((2, part, width), LOW), vmem((2, 2, part, width), LOW), vmem((part, width), F32), vmem((BAND, width), F32),
            vmem((1, width), F32), vmem((GROUP, 1, width), F32),
            vmem((2, ROWS, rows), LOW), vmem((2, rows, ROWS), LOW), vmem((2, 3, ROWS, ROWS), LOW), vmem((2, ROWS, ROWS), LOW),
            dma((10,)), dma((2, 2)), dma((2, 2)), dma((2, 2)), dma((2, 2, 2)), dma((GROUP - 1,)), dma((GROUP - 1,)),
            dma((2,)), dma((2,)), dma((2, 3)), dma((2,)),
        ],
        compiler_params=pltpu.CompilerParams(collective_id=0, has_side_effects=True, vmem_limit_bytes=VMEM),
        cost_estimate=pl.CostEstimate(flops=2 * rows * width * ROWS * 7, transcendentals=0, bytes_accessed=rows * width * 6),
    )(dq, dk, dv, wq, wk, wv, at, dy, seen, x, my_dy, gain)


def _keep(*refs):
    given, kept, (held, in_sem, out_sem) = refs[:6], refs[6:12], (refs[12:18], *refs[18:])
    ins = [pltpu.make_async_copy(a, b, in_sem.at[n]) for n, (a, b) in enumerate(zip(given, held))]
    outs = [pltpu.make_async_copy(a, b, out_sem.at[n]) for n, (a, b) in enumerate(zip(held, kept))]
    for copy in ins:
        copy.start()
    for a, b in zip(ins, outs):
        a.wait()
        b.start()
    for copy in outs:
        copy.wait()


def keep(results):
    count = len(results)
    return pl.pallas_call(
        _keep,
        in_specs=[ANY] * count,
        out_specs=[ANY] * count,
        out_shape=[jax.ShapeDtypeStruct(r.shape, r.dtype) for r in results],
        scratch_shapes=[*(pltpu.VMEM(r.shape, r.dtype) for r in results), *[pltpu.SemaphoreType.DMA((count,))] * 2],
        compiler_params=pltpu.CompilerParams(vmem_limit_bytes=VMEM),
    )(*results)


def tables(rows):
    half = HEAD // 2
    rate = float(THETA) ** (-(np.arange(HEAD) % half) / half)
    turns = [np.arange(0, rows, ANGLES)[:, None] * rate, np.arange(ANGLES)[:, None] * rate]
    return [jnp.asarray(np.stack([np.cos(t), np.sin(t)]), F32) for t in turns]


HALF = ROWS // 2
SPAN = 4 * HALF
QUERIES = 1024


def _gather(x_h, dy_h, gain, wq_h, wk_h, wv_h, wo_h, far, near, all_h, at_h, dq_h, dk_h, dv_h, out_h,
            x_s, mine, w, wo, lhs, turned_s, q, k, v, by, out, lse, top_s, mix_s, gap_s, asked_s, facts_s, dq_s, dk_s, dv_s, lag_s,
            load_sem, store_sem, hop_send, hop_recv, swap_send, swap_recv, lhs_sem, at_sem, result_sem):
    me = lax.axis_index("tp")
    chip, core = me // 2, me % 2
    place = _ring_chip(chip)
    twin = 2 * chip + 1 - core
    ways = [2 * _ring_chip((place + d) % CHIPS) + core for d in (1, CHIPS - 1)]
    barrier = pltpu.get_barrier_semaphore()
    for other in (twin, *ways):
        pl.semaphore_signal(barrier, inc=1, device_id={"tp": other}, device_id_type=MESH)
    part = [slice(n * ROWS, (n + 1) * ROWS) for n in range(3)]
    width = x_s.shape[1]
    heads, bq, bk, scale = ROWS // HEAD, QUERIES, KEYS, HEAD**-0.5
    e = scale * LOG2E

    given = ((x_h, x_s), (dy_h, lhs.at[0, :ROWS, :]), *((a, w.at[:, here]) for a, here in zip((wq_h, wk_h, wv_h), part)), (wo_h, wo))
    loads = [pltpu.make_async_copy(a, b, load_sem.at[n]) for n, (a, b) in enumerate(given)]
    for load in loads:
        load.start()
    here = pl.ds(pl.multiple_of(me * ROWS, ROWS), ROWS)
    stores = [pltpu.make_async_copy(a, all_h.at[n, here, :], store_sem.at[n]) for n, a in enumerate((mine, lhs.at[0, :ROWS, :]))]
    loads[0].wait()

    def norm(j, _):
        band = pl.ds(pl.multiple_of(j * BAND, BAND), BAND)
        wide = x_s[band, :].astype(F32)
        mine[band, :] = (wide * lax.rsqrt(jnp.mean(wide * wide, -1, keepdims=True) + EPS) * gain[...].astype(F32)).astype(LOW)

    lax.fori_loop(0, ROWS // BAND, norm, None)
    stores[0].start()
    loads[1].wait()
    stores[1].start()
    for store in stores:
        store.wait()
    pl.semaphore_wait(barrier, 3)

    def begins(way, g):
        return _ring_chip((place + (g if way else 2 * CHIPS - g)) % CHIPS)

    def piece(p, g, way, c, of):
        start = (2 * begins(way, g) + of) * ROWS + way * HALF + c * STEP
        return all_h.at[p, pl.ds(pl.multiple_of(start, STEP), STEP), :]

    def hop(p, g, way, c):
        rows = piece(p, g, way, c, core)
        return pltpu.make_async_remote_copy(src_ref=rows, dst_ref=rows, send_sem=hop_send.at[p, g, way, c], recv_sem=hop_recv.at[p, g, way, c],
                                            device_id={"tp": ways[way]}, device_id_type=MESH)

    def arrival(p, g, way, c):
        rows = piece(p, g, way, c, core)
        return pltpu.make_async_remote_copy(src_ref=rows, dst_ref=rows, send_sem=hop_send.at[p, g - 1, way, c],
                                            recv_sem=hop_recv.at[p, g - 1, way, c], device_id={"tp": ways[way]}, device_id_type=MESH)

    def swap(p, g, way, c, of):
        rows = piece(p, g, way, c, of)
        return pltpu.make_async_remote_copy(src_ref=rows, dst_ref=rows, send_sem=swap_send.at[p, g, way, c], recv_sem=swap_recv.at[p, g, way, c],
                                            device_id={"tp": twin}, device_id_type=MESH)

    def starts(g):
        return [(2 * begins(way, g) + of) * ROWS + way * HALF for way in range(2) for of in range(2)]

    def fetch(n):
        return [pltpu.make_async_copy(all_h.at[n // CHIPS, pl.ds(pl.multiple_of(start, HALF), HALF), :],
                                      lhs.at[n % 2, i * HALF : (i + 1) * HALF, :], lhs_sem.at[n % 2, i]) for i, start in enumerate(starts(n % CHIPS))]

    def put(g):
        return [pltpu.make_async_copy(turned_s.at[:, i * HALF : (i + 1) * HALF], at_h.at[:, pl.ds(pl.multiple_of(start, HALF), HALF)], at_sem.at[i])
                for i, start in enumerate(starts(g))]

    def project(n):
        begin = starts(n % CHIPS)
        for m, to in enumerate((q, k, v)):
            got = _dot(lhs[n % 2], w[:, part[m]], 1, 0).astype(LOW)
            for i, start in enumerate(begin):
                rows = pl.ds(pl.multiple_of(start, HALF), HALF)
                angle = _angle(start // ANGLES, far, near)
                for h in range(heads):
                    t = got[i * HALF : (i + 1) * HALF, _head(h)]
                    to[rows, _head(h)] = t if m == 2 else _turn(t, angle, 0)

    def turn_over(n):
        @pl.when(n > 0)
        def _():
            for copy in put(n - 1):
                copy.wait()

        def columns(j, _):
            here = pl.ds(pl.multiple_of(j * STRIP, STRIP), STRIP)
            turned_s[here, :] = lhs[n % 2, :, here].T

        lax.fori_loop(0, width // STRIP, columns, None)
        for copy in put(n):
            copy.start()

    def products(n):
        by[n % CHIPS] = _dot(lhs[n % 2], wo[...], 1, 1).astype(LOW)

    def block(iq, j, masked):
        ones = jnp.ones((8, bk), LOW)
        keys = pl.ds(pl.multiple_of(j * bk, bk), bk)
        pieces = _pieces(heads, bq)
        asked = [pl.ds(pl.multiple_of(iq * bq + at.start, STRIP), STRIP) for _, at in pieces]
        scores = [_dot(k[keys, _head(i)], q[rows, _head(i)], 1, 1) for (i, _), rows in zip(pieces, asked)]
        ok = gap_s[...] >= j * bk - iq * bq if masked else None
        weights, keeps = [], []
        for (i, at), s in zip(pieces, scores):
            if masked:
                s = jnp.where(ok[:, at], s, HIDDEN)
            old = top_s[i : i + 1, at]
            top = jnp.maximum(old, s.max(axis=0, keepdims=True))
            top_s[i : i + 1, at] = top
            weights.append(jnp.exp2((s - top) * e).astype(LOW))
            keeps.append(jnp.exp2((old - top) * e))
        for (i, at), p, keep in zip(pieces, weights, keeps):
            values = jnp.concatenate([v[keys, _head(i)].T, ones], axis=0)
            mix_s[i, :, at] = mix_s[i, :, at] * keep + _dot(values, p, 1, 0)

    per = bq // bk
    count = width // bq
    total = per * count * (count + 1) // 2

    def attend(n):
        iq = sum((n >= per * i * (i + 1) // 2).astype(jnp.int32) for i in range(1, count))
        j = n - per * iq * (iq + 1) // 2

        @pl.when(j == 0)
        def _():
            top_s[...] = jnp.full_like(top_s, NEG)
            mix_s[...] = jnp.zeros_like(mix_s)

        @pl.when(j < per * iq)
        def _():
            block(iq, j, False)

        @pl.when(j >= per * iq)
        def _():
            block(iq, j, True)

        @pl.when(j == per * (iq + 1) - 1)
        def _():
            rows = pl.ds(pl.multiple_of(iq * bq, bq), bq)
            for i in range(heads):
                top, weight = top_s[i : i + 1, :], mix_s[i, HEAD : HEAD + 1, :]
                out[_head(i), rows] = (mix_s[i, :HEAD, :] * (1 / weight)).astype(LOW)
                lse[i : i + 1, rows] = top * scale + jnp.log(weight)

    def back(ways, g, j, masked):
        keys = pl.ds(pl.multiple_of(j * bk, bk), bk)
        pieces = [(way, i) for way in ways for i in range(heads)]
        qs = [asked_s[way, :, _head(i)] for way, i in pieces]
        dos = [by[g, pl.ds(pl.multiple_of(way * ROWS, ROWS), ROWS), _head(i)] for way, i in pieces]
        scores = [_dot(k[keys, _head(i)], x, 1, 1) for (_, i), x in zip(pieces, qs)]
        dps = [_dot(v[keys, _head(i)], x, 1, 1) for (_, i), x in zip(pieces, dos)]
        for n, (way, i) in enumerate(pieces):
            p = jnp.exp2(scores[n] * e - facts_s[way, i : i + 1, :])
            if masked:
                p = jnp.where(lag_s[...] >= -HALF * way, p, 0.0)
            ds = (p * (dps[n] - facts_s[way, heads + i : heads + i + 1, :])).astype(LOW)
            dv_s[i, keys, :] += _dot(p.astype(LOW), dos[n], 1, 0)
            dk_s[i, keys, :] += _dot(ds, qs[n], 1, 0)
            dq_s[way, i] += _dot(k[keys, _head(i)].T, ds, 1, 0)

    def backward(g):
        begin = starts(g)
        dq_s[...] = jnp.zeros_like(dq_s)
        for n, start in enumerate(begin):
            rows, way = pl.ds(pl.multiple_of(start, HALF), HALF), n // 2
            at = slice(n % 2 * HALF, (n % 2 + 1) * HALF)
            asked_s[way, at, :] = q[rows, :]
            for i in range(heads):
                facts_s[way, i : i + 1, at] = lse[i : i + 1, rows] * LOG2E
                d_out = by[g, n * HALF : (n + 1) * HALF, _head(i)].astype(F32).T
                facts_s[way, heads + i : heads + i + 1, at] = (d_out * out[_head(i), rows].astype(F32)).sum(0, keepdims=True)
        ends = [begins(way, g) for way in range(2)]
        least, most = jnp.minimum(*ends), jnp.maximum(*ends)
        late = (ends[1] > ends[0]).astype(jnp.int32)
        lax.fori_loop(0, least, lambda j, _: back((0, 1), g, j, False), None)
        lax.fori_loop(least, most, lambda j, _: back((late,), g, j, False), None)
        lax.fori_loop(0, 2, lambda way, _: back((way,), g, jnp.where(way == late, most, least), True), None)
        for n, start in enumerate(begin):
            rows, way = pl.ds(pl.multiple_of(start, HALF), HALF), n // 2
            angle = _angle(start // ANGLES, far, near)
            for i in range(heads):
                q[rows, _head(i)] = _turn((dq_s[way, i, :, n % 2 * HALF : (n % 2 + 1) * HALF] * scale).T, angle, 1)

    steps = 2 * CHIPS
    first, share = steps + 1, 4
    began = first + total // share

    def work(m, n, c):
        @pl.when(m == 0)
        def _():
            gap_s[...] = _gap(bk, bq)
            column = lax.broadcasted_iota(jnp.int32, lag_s.shape, 1)
            lag_s[...] = column + jnp.where(column >= HALF, HALF, 0) - lax.broadcasted_iota(jnp.int32, lag_s.shape, 0)
            dk_s[...] = jnp.zeros_like(dk_s)
            dv_s[...] = jnp.zeros_like(dv_s)
            for load in loads[2:]:
                load.wait()

        @pl.when((c == 0) & (n > 0))
        def _():
            for copy in fetch(n - 1):
                copy.wait()

            @pl.when(n <= CHIPS)
            def _():
                project(n - 1)

            @pl.when(n > CHIPS)
            def _():
                products(n - 1)

        @pl.when((c == 1) & (n > 0) & (n <= CHIPS))
        def _():
            turn_over(n - 1)

        @pl.when((m >= first) & (m < began))
        def _():
            lax.fori_loop(share * (m - first), share * (m - first + 1), lambda i, _: attend(i), None)

        @pl.when((m >= began) & ((m <= began + share) | (c == 0)))
        def _():
            backward(jnp.where(m <= began + share, m - began, n - CHIPS - 1))

        @pl.when((c == 1) & (n < steps))
        def _():
            for way in range(2):
                for i in range(2):
                    swap(n // CHIPS, n % CHIPS, way, i, 1 - core).wait_recv()
            for copy in fetch(n):
                copy.start()

    def step(m, _):
        n, c = m // 2, m % 2
        p, g = n // CHIPS, n % CHIPS

        @pl.when((g > 0) & (n < steps))
        def _():
            for way in range(2):
                arrival(p, g, way, c).wait_recv()

        @pl.when((n != CHIPS) & (n < steps - 1))
        def _():
            for way in range(2):
                hop(jnp.where(n == CHIPS - 1, 1, p), jnp.where(n == CHIPS - 1, 0, g), way, c).start()

        @pl.when(n < steps)
        def _():
            for way in range(2):
                swap(p, g, way, c, core).start()

        work(m, n, c)

    lax.fori_loop(0, 2 * steps + 1, step, None)

    def finish(j, _):
        here = pl.ds(pl.multiple_of(j * ANGLES, ANGLES), ANGLES)
        angle = _angle(j, far, near)
        for i in range(heads):
            k[here, _head(i)] = _turn(dk_s[i, here, :] * scale, angle, 1)
            v[here, _head(i)] = dv_s[i, here, :].astype(LOW)

    quarters = [slice(n * QUERIES, (n + 1) * QUERIES) for n in range(count)]
    given = ((out, out_h), (q, dq_h), *((a.at[at, :], b.at[at, :]) for at in quarters for a, b in ((k, dk_h), (v, dv_h))))
    results = [pltpu.make_async_copy(a, b, result_sem.at[n]) for n, (a, b) in enumerate(given)]
    for copy in results[:2]:
        copy.start()
    for n in range(count):
        per = QUERIES // ANGLES
        lax.fori_loop(per * n, per * (n + 1), finish, None)
        for copy in results[2 * n + 2 : 2 * n + 4]:
            copy.start()

    def sent(n, _):
        p, g = n // CHIPS, n % CHIPS
        for way in range(2):
            for c in range(2):
                swap(p, g, way, c, core).wait_send()

                @pl.when(g < CHIPS - 1)
                def _():
                    hop(p, g, way, c).wait_send()

    lax.fori_loop(0, steps, sent, None)
    for copy in put(CHIPS - 1):
        copy.wait()
    for copy in results:
        copy.wait()


def gather(x, dy, gain, wq, wk, wv, wo, far, near):
    width, rows = x.shape[1], GROUP * ROWS
    heads = ROWS // HEAD
    vmem, dma = pltpu.VMEM, pltpu.SemaphoreType.DMA
    here = pl.BlockSpec(memory_space=pltpu.VMEM)
    by_token, by_head, sums = (rows, ROWS), (ROWS, rows), (heads, rows, HEAD)
    shapes = [(2, rows, width), (width, rows), by_token, by_token, by_token, by_head]
    return pl.pallas_call(
        _gather,
        in_specs=[ANY, ANY, here, ANY, ANY, ANY, ANY, here, here],
        out_specs=[ANY] * len(shapes),
        out_shape=[jax.ShapeDtypeStruct(shape, LOW) for shape in shapes],
        scratch_shapes=[
            vmem(x.shape, LOW), vmem(x.shape, LOW), vmem((width, 3 * ROWS), LOW), vmem((ROWS, width), LOW), vmem((2, SPAN, width), LOW),
            vmem((width, SPAN), LOW), *[vmem(by_token, LOW)] * 3, vmem((CHIPS, SPAN, ROWS), LOW), vmem(by_head, LOW), vmem((heads, rows), F32),
            vmem((heads, QUERIES), F32), vmem((heads, HEAD + 8, QUERIES), F32), vmem((KEYS, QUERIES), jnp.int32),
            vmem((2, ROWS, ROWS), LOW), vmem((2, 2 * heads, ROWS), F32), vmem((2, heads, HEAD, ROWS), F32), vmem(sums, F32), vmem(sums, F32),
            vmem((KEYS, ROWS), jnp.int32),
            dma((6,)), dma((2,)), *[dma((2, CHIPS, 2, 2))] * 4, dma((2, 4)), dma((4,)), dma((10,)),
        ],
        compiler_params=pltpu.CompilerParams(collective_id=1, has_side_effects=True, vmem_limit_bytes=VMEM),
        cost_estimate=pl.CostEstimate(flops=2 * rows * width * ROWS * 8, transcendentals=rows * rows, bytes_accessed=rows * width * 8),
    )(x, dy, gain, wq, wk, wv, wo, far, near)

def solution(mesh):
    def step(x, dy, gain, wq, wk, wv, wo):
        gain = gain[None]
        far, near = tables(GROUP * ROWS)
        gathered, at, dq, dk, dv, out = gather(x, dy, gain, wq, wk, wv, wo, far, near)
        return tuple(keep(scatter(dq, dk, dv, wq, wk, wv, at, gathered, out, x, dy, gain)))

    tokens, columns = P(("dp", "tp"), None), P(None, "tp")
    return jax.shard_map(
        step,
        mesh=mesh,
        in_specs=(tokens, tokens, P(None), columns, columns, columns, P("tp", None)),
        out_specs=(tokens, P("dp", None), P("dp", "tp"), P("dp", "tp"), P("dp", "tp"), P(("dp", "tp"), None)),
        check_vma=False,
    )
```

```python
import functools

import jax
import jax.numpy as jnp
import numpy as np
from jax import lax
from jax.experimental import pallas as pl
from jax.experimental.pallas import tpu as pltpu
from jax.sharding import PartitionSpec as P

NEG = -1e30
HIDDEN = 2 * NEG
LOG2E = 1.4426950408889634
VMEM = 62 * 2**20
STRIP = 512
KEYS = 512
HEAD = 128
THETA = 10000
ANGLES = 128
EPS = 1e-6
MESH = pl.DeviceIdType.MESH
ANY = pl.BlockSpec(memory_space=pl.ANY)
LOW = jnp.bfloat16
F32 = jnp.float32


def _dot(a, b, ca, cb):
    return lax.dot_general(a, b, (((ca,), (cb,)), ((), ())), preferred_element_type=F32)


def _gap(bk, bq):
    return lax.broadcasted_iota(jnp.int32, (bk, bq), 1) - lax.broadcasted_iota(jnp.int32, (bk, bq), 0)


def _head(i):
    return slice(i * HEAD, (i + 1) * HEAD)


def _pieces(heads, bq):
    return [(i, slice(at, at + STRIP)) for i in range(heads) for at in range(0, bq, STRIP)]


def _angle(m, far, near):
    here = pl.ds(m, 1)
    cos = far[0, here, :] * near[0] - far[1, here, :] * near[1]
    sin = far[1, here, :] * near[0] + far[0, here, :] * near[1]
    return cos, jnp.where(lax.broadcasted_iota(jnp.int32, sin.shape, 1) < HEAD // 2, sin, -sin)


def _turn(t, angle, way):
    cos, sin = angle
    t = t.astype(LOW).astype(F32)
    swapped = pltpu.roll(t, HEAD // 2, 1) * sin
    return (t * cos + (swapped if way else -swapped)).astype(LOW)


GROUP = 16
CHIPS = GROUP // 2
ROWS = 256
STEP = ROWS // 4
BAND = 16


def _ring_chip(place):
    return jnp.where(place < CHIPS // 2, place, CHIPS + CHIPS // 2 - 1 - place)


def _greet(others):
    barrier = pltpu.get_barrier_semaphore()
    for other in others:
        pl.semaphore_signal(barrier, inc=1, device_id={"tp": other}, device_id_type=MESH)
    pl.semaphore_wait(barrier, len(others))


def _scatter(dq_h, dk_h, dv_h, wq_h, wk_h, wv_h, at_h, dy_h, seen_h, x_h, my_dy_h, gain_h, dx_ref, dgain_ref, dwq_h, dwk_h, dwv_h, dwo_h,
             dqkv, w, seen, x_s, my_dy, gain, lhs, own, twin_out, twin_in, ring_out, ring_in, total_s, unit_sum, gain_out, gain_in,
             at_s, dy_s, dw_s, dwo_s,
             load_sem, twin_send, twin_recv, ring_send, ring_recv, gain_send, gain_recv, at_sem, dy_sem, dw_sem, dwo_sem):
    me = lax.axis_index("tp")
    chip, core = me // 2, me % 2
    place = _ring_chip(chip)
    twin = 2 * chip + 1 - core
    after = 2 * _ring_chip((place + 1) % CHIPS) + core
    before = 2 * _ring_chip((place + CHIPS - 1) % CHIPS) + core
    width = w.shape[0]
    part = [slice(n * ROWS, (n + 1) * ROWS) for n in range(3)]

    given = (*((a, dqkv.at[:, here]) for a, here in zip((dq_h, dk_h, dv_h), part)), *((a, w.at[:, here]) for a, here in zip((wq_h, wk_h, wv_h), part)),
             (seen_h, seen), (x_h, x_s), (my_dy_h, my_dy), (gain_h, gain))
    loads = [pltpu.make_async_copy(a, b, load_sem.at[n]) for n, (a, b) in enumerate(given)]
    for load in loads[:6]:
        load.start()

    def fetch(u, slot):
        here = pl.ds(pl.multiple_of(u * ROWS, ROWS), ROWS)
        return (pltpu.make_async_copy(at_h.at[here, :], at_s.at[slot], at_sem.at[slot]),
                pltpu.make_async_copy(dy_h.at[1, :, here], dy_s.at[slot], dy_sem.at[slot]))

    def put(u, slot):
        here = pl.ds(pl.multiple_of(u * ROWS, ROWS), ROWS)
        return (*(pltpu.make_async_copy(dw_s.at[slot, n], out.at[here, :], dw_sem.at[slot, n]) for n, out in enumerate((dwq_h, dwk_h, dwv_h))),
                pltpu.make_async_copy(dwo_s.at[slot], dwo_h.at[:, here], dwo_sem.at[slot]))

    others = [(me + d) % GROUP for d in range(1, GROUP)]
    _greet(others)

    def swap(slot, c):
        return pltpu.make_async_remote_copy(src_ref=twin_out.at[slot, c], dst_ref=twin_in.at[slot, c], send_sem=twin_send.at[slot, c],
                                            recv_sem=twin_recv.at[slot, c], device_id={"tp": twin}, device_id_type=MESH)

    def hop(slot, way, c):
        here = pl.ds(way * STEP, STEP)
        return pltpu.make_async_remote_copy(src_ref=ring_out.at[c, here, :], dst_ref=ring_in.at[slot, c, here, :], send_sem=ring_send.at[way, c],
                                            recv_sem=ring_recv.at[slot, way, c], device_id={"tp": before if way else after}, device_id_type=MESH)

    def terms(s, c):
        forth = _ring_chip((place + 2 * CHIPS - 1 - s) % CHIPS)
        back = _ring_chip((place + 1 + s) % CHIPS)
        starts = [(2 * to + of) * ROWS + (2 * way + c) * STEP for of in (core, 1 - core) for way, to in ((0, forth), (1, back))]
        for n, start in enumerate(starts):
            lhs[n * STEP : (n + 1) * STEP, :] = dqkv[pl.ds(pl.multiple_of(start, STEP), STEP), :]
        slot = s % 2

        def columns(j, _):
            here = pl.ds(pl.multiple_of(j * STRIP, STRIP), STRIP)
            term = _dot(lhs[...], w[here, :], 1, 1)
            own[c, :, here] = term[: 2 * STEP]
            twin_out[slot, c, :, here] = term[2 * STEP :].astype(LOW)

        lax.fori_loop(0, width // STRIP, columns, None)
        swap(slot, c).start()

    def add(s, c, ringed, last):
        slot = s % 2

        def columns(j, _):
            here = pl.ds(pl.multiple_of(j * ROWS, ROWS), ROWS)
            total = own[c, :, here] + twin_in[slot, c, :, here].astype(F32)
            if ringed:
                total += ring_in[1 - slot, c, :, here].astype(F32)
            if last:
                total_s[:, here] = total
            else:
                ring_out[c, :, here] = total.astype(LOW)

        lax.fori_loop(0, width // ROWS, columns, None)

    def norm(c):
        def band(j, _):
            src = pl.ds(pl.multiple_of(j * BAND, BAND), BAND)
            at = c * STEP + j * BAND + jnp.where(j >= STEP // BAND, STEP, 0)
            dst = pl.ds(pl.multiple_of(at, BAND), BAND)
            wide, by = x_s[dst, :].astype(F32), total_s[src, :]
            scale = lax.rsqrt(jnp.mean(wide * wide, -1, keepdims=True) + EPS)
            unit = wide * scale
            unit_sum[...] += by * unit
            by = by * gain[...].astype(F32)
            dx = scale * (by - unit * jnp.mean(by * unit, -1, keepdims=True))
            dx_ref[dst, :] = (my_dy[dst, :].astype(F32) + dx).astype(LOW)

        lax.fori_loop(0, 2 * STEP // BAND, band, None)

    def weights(u, slot):
        for copy in fetch(u, slot):
            copy.wait()

        @pl.when(u < GROUP - 1)
        def _():
            for copy in fetch(u + 1, 1 - slot):
                copy.start()

        @pl.when(u >= 2)
        def _():
            for copy in put(u, slot):
                copy.wait()

        for n in range(3):
            dw_s[slot, n] = _dot(at_s[slot], dqkv[:, part[n]], 1, 0).astype(LOW)
        dwo_s[slot] = _dot(seen[...], dy_s[slot], 1, 0).astype(LOW)
        for copy in put(u, slot):
            copy.start()

    for load in loads[:6]:
        load.wait()
    for load in loads[6:]:
        load.start()
    for copy in fetch(0, 0):
        copy.start()
    terms(0, 0)
    for load in loads[6:]:
        load.wait()
    unit_sum[...] = jnp.zeros_like(unit_sum)
    last = CHIPS - 1

    def step(s, _):
        slot = s % 2
        for c in range(2):
            swap(slot, c).wait_recv()

            @pl.when(s == 0)
            def _():
                add(s, c, False, False)

            @pl.when(s > 0)
            def _():
                for way in range(2):
                    hop(1 - slot, way, c).wait()
                add(s, c, True, False)

            for way in range(2):
                hop(slot, way, c).start()
            if c == 0:
                @pl.when(s == 0)
                def _():
                    terms(0, 1)

            @pl.when(s > 0)
            def _():
                swap(1 - slot, c).wait_send()

            terms(s + 1, c)
            weights(2 * s + c, c)

    lax.fori_loop(0, last, step, None)
    for c in range(2):
        swap(last % 2, c).wait_recv()
        for way in range(2):
            hop(1 - last % 2, way, c).wait()
        add(last, c, True, True)
        norm(c)
        if c == 0:
            weights(2 * last, c)
    gain_out[...] = unit_sum[...].sum(0, keepdims=True)
    gain_in[me] = gain_out[...]
    copies = [pltpu.make_async_remote_copy(src_ref=gain_out, dst_ref=gain_in.at[me], send_sem=gain_send.at[n], recv_sem=gain_recv.at[n],
                                           device_id={"tp": other}, device_id_type=MESH) for n, other in enumerate(others)]
    for copy in copies:
        copy.start()
    weights(2 * last + 1, 1)
    for copy in copies:
        copy.wait()
    dgain_ref[...] = functools.reduce(lambda a, b: a + b, [gain_in[n] for n in range(GROUP)])
    for c in range(2):
        for slot in range(2):
            swap(slot, c).wait_send()
        for copy in put(2 * last + c, c):
            copy.wait()


def scatter(dq, dk, dv, wq, wk, wv, at, dy, seen, x, my_dy, gain):
    width, rows = at.shape
    vmem, dma = pltpu.VMEM, pltpu.SemaphoreType.DMA
    here = pl.BlockSpec(memory_space=pltpu.VMEM)
    part, mine = 2 * STEP, (ROWS, width)
    by_weight = jax.ShapeDtypeStruct((width, ROWS), LOW)
    return pl.pallas_call(
        _scatter,
        in_specs=[ANY] * 12,
        out_specs=[here] * 2 + [ANY] * 4,
        out_shape=[jax.ShapeDtypeStruct(mine, LOW), jax.ShapeDtypeStruct((1, width), F32)] + [by_weight] * 3 + [jax.ShapeDtypeStruct(mine, LOW)],
        scratch_shapes=[
            vmem((rows, 3 * ROWS), LOW), vmem((width, 3 * ROWS), LOW), vmem(seen.shape, LOW), vmem(mine, LOW), vmem(mine, LOW), vmem((1, width), LOW),
            vmem((4 * STEP, 3 * ROWS), LOW),
            vmem((2, part, width), F32), vmem((2, 2, part, width), LOW), vmem((2, 2, part, width), LOW),
            vmem((2, part, width), LOW), vmem((2, 2, part, width), LOW), vmem((part, width), F32), vmem((BAND, width), F32),
            vmem((1, width), F32), vmem((GROUP, 1, width), F32),
            vmem((2, ROWS, rows), LOW), vmem((2, rows, ROWS), LOW), vmem((2, 3, ROWS, ROWS), LOW), vmem((2, ROWS, ROWS), LOW),
            dma((10,)), dma((2, 2)), dma((2, 2)), dma((2, 2)), dma((2, 2, 2)), dma((GROUP - 1,)), dma((GROUP - 1,)),
            dma((2,)), dma((2,)), dma((2, 3)), dma((2,)),
        ],
        compiler_params=pltpu.CompilerParams(collective_id=0, has_side_effects=True, vmem_limit_bytes=VMEM),
        cost_estimate=pl.CostEstimate(flops=2 * rows * width * ROWS * 7, transcendentals=0, bytes_accessed=rows * width * 6),
    )(dq, dk, dv, wq, wk, wv, at, dy, seen, x, my_dy, gain)


def _keep(*refs):
    given, kept, (held, in_sem, out_sem) = refs[:6], refs[6:12], (refs[12:18], *refs[18:])
    ins = [pltpu.make_async_copy(a, b, in_sem.at[n]) for n, (a, b) in enumerate(zip(given, held))]
    outs = [pltpu.make_async_copy(a, b, out_sem.at[n]) for n, (a, b) in enumerate(zip(held, kept))]
    for copy in ins:
        copy.start()
    for a, b in zip(ins, outs):
        a.wait()
        b.start()
    for copy in outs:
        copy.wait()


def keep(results):
    count = len(results)
    return pl.pallas_call(
        _keep,
        in_specs=[ANY] * count,
        out_specs=[ANY] * count,
        out_shape=[jax.ShapeDtypeStruct(r.shape, r.dtype) for r in results],
        scratch_shapes=[*(pltpu.VMEM(r.shape, r.dtype) for r in results), *[pltpu.SemaphoreType.DMA((count,))] * 2],
        compiler_params=pltpu.CompilerParams(vmem_limit_bytes=VMEM),
    )(*results)


def tables(rows):
    half = HEAD // 2
    rate = float(THETA) ** (-(np.arange(HEAD) % half) / half)
    turns = [np.arange(0, rows, ANGLES)[:, None] * rate, np.arange(ANGLES)[:, None] * rate]
    return [jnp.asarray(np.stack([np.cos(t), np.sin(t)]), F32) for t in turns]


HALF = ROWS // 2
SPAN = 4 * HALF
QUERIES = 1024


def _gather(x_h, dy_h, gain, wq_h, wk_h, wv_h, wo_h, far, near, all_h, at_h, dq_h, dk_h, dv_h, out_h,
            x_s, mine, w, wo, lhs, turned_s, q, k, v, by, out, lse, top_s, mix_s, gap_s, asked_s, facts_s, dq_s, dk_s, dv_s, lag_s,
            load_sem, store_sem, hop_send, hop_recv, swap_send, swap_recv, lhs_sem, at_sem, result_sem):
    me = lax.axis_index("tp")
    chip, core = me // 2, me % 2
    place = _ring_chip(chip)
    twin = 2 * chip + 1 - core
    ways = [2 * _ring_chip((place + d) % CHIPS) + core for d in (1, CHIPS - 1)]
    barrier = pltpu.get_barrier_semaphore()
    for other in (twin, *ways):
        pl.semaphore_signal(barrier, inc=1, device_id={"tp": other}, device_id_type=MESH)
    part = [slice(n * ROWS, (n + 1) * ROWS) for n in range(3)]
    width = x_s.shape[1]
    heads, bq, bk, scale = ROWS // HEAD, QUERIES, KEYS, HEAD**-0.5
    e = scale * LOG2E

    given = ((x_h, x_s), (dy_h, lhs.at[0, :ROWS, :]), *((a, w.at[:, here]) for a, here in zip((wq_h, wk_h, wv_h), part)), (wo_h, wo))
    loads = [pltpu.make_async_copy(a, b, load_sem.at[n]) for n, (a, b) in enumerate(given)]
    for load in loads:
        load.start()
    stores = [pltpu.make_async_copy(mine.at[at, :], all_h.at[0, pl.ds(pl.multiple_of(me * ROWS + at.start, STEP), STEP), :], store_sem.at[n])
              for n, at in enumerate(slice(way * HALF + c * STEP, way * HALF + (c + 1) * STEP) for c in range(2) for way in range(2))]
    stores += [pltpu.make_async_copy(lhs.at[0, :ROWS, :], all_h.at[1, pl.ds(pl.multiple_of(me * ROWS, ROWS), ROWS), :], store_sem.at[4])]
    loads[0].wait()

    def norm(c):
        def band(j, _):
            at = c * STEP + j * BAND + jnp.where(j >= STEP // BAND, HALF - STEP, 0)
            rows = pl.ds(pl.multiple_of(at, BAND), BAND)
            wide = x_s[rows, :].astype(F32)
            mine[rows, :] = (wide * lax.rsqrt(jnp.mean(wide * wide, -1, keepdims=True) + EPS) * gain[...].astype(F32)).astype(LOW)

        lax.fori_loop(0, 2 * STEP // BAND, band, None)
        for store in stores[2 * c : 2 * c + 2]:
            store.start()

    norm(0)
    for store in stores[:2]:
        store.wait()
    pl.semaphore_wait(barrier, 3)

    def begins(way, g):
        return _ring_chip((place + (g if way else 2 * CHIPS - g)) % CHIPS)

    def piece(p, g, way, c, of):
        start = (2 * begins(way, g) + of) * ROWS + way * HALF + c * STEP
        return all_h.at[p, pl.ds(pl.multiple_of(start, STEP), STEP), :]

    def hop(p, g, way, c):
        rows = piece(p, g, way, c, core)
        return pltpu.make_async_remote_copy(src_ref=rows, dst_ref=rows, send_sem=hop_send.at[p, g, way, c], recv_sem=hop_recv.at[p, g, way, c],
                                            device_id={"tp": ways[way]}, device_id_type=MESH)

    def arrival(p, g, way, c):
        rows = piece(p, g, way, c, core)
        return pltpu.make_async_remote_copy(src_ref=rows, dst_ref=rows, send_sem=hop_send.at[p, g - 1, way, c],
                                            recv_sem=hop_recv.at[p, g - 1, way, c], device_id={"tp": ways[way]}, device_id_type=MESH)

    def swap(p, g, way, c, of):
        rows = piece(p, g, way, c, of)
        return pltpu.make_async_remote_copy(src_ref=rows, dst_ref=rows, send_sem=swap_send.at[p, g, way, c], recv_sem=swap_recv.at[p, g, way, c],
                                            device_id={"tp": twin}, device_id_type=MESH)

    def starts(g):
        return [(2 * begins(way, g) + of) * ROWS + way * HALF for way in range(2) for of in range(2)]

    def fetch(n):
        return [pltpu.make_async_copy(all_h.at[n // CHIPS, pl.ds(pl.multiple_of(start, HALF), HALF), :],
                                      lhs.at[n % 2, i * HALF : (i + 1) * HALF, :], lhs_sem.at[n % 2, i]) for i, start in enumerate(starts(n % CHIPS))]

    def put(g):
        return [pltpu.make_async_copy(turned_s.at[:, i * HALF : (i + 1) * HALF], at_h.at[:, pl.ds(pl.multiple_of(start, HALF), HALF)], at_sem.at[i])
                for i, start in enumerate(starts(g))]

    def project(n):
        begin = starts(n % CHIPS)
        for m, to in enumerate((q, k, v)):
            got = _dot(lhs[n % 2], w[:, part[m]], 1, 0).astype(LOW)
            for i, start in enumerate(begin):
                rows = pl.ds(pl.multiple_of(start, HALF), HALF)
                angle = _angle(start // ANGLES, far, near)
                for h in range(heads):
                    t = got[i * HALF : (i + 1) * HALF, _head(h)]
                    to[rows, _head(h)] = t if m == 2 else _turn(t, angle, 0)

    def turn_over(n):
        @pl.when(n > 0)
        def _():
            for copy in put(n - 1):
                copy.wait()

        def columns(j, _):
            here = pl.ds(pl.multiple_of(j * STRIP, STRIP), STRIP)
            turned_s[here, :] = lhs[n % 2, :, here].T

        lax.fori_loop(0, width // STRIP, columns, None)
        for copy in put(n):
            copy.start()

    def products(n):
        by[n % CHIPS] = _dot(lhs[n % 2], wo[...], 1, 1).astype(LOW)

    def block(iq, j, masked):
        ones = jnp.ones((8, bk), LOW)
        keys = pl.ds(pl.multiple_of(j * bk, bk), bk)
        pieces = _pieces(heads, bq)
        asked = [pl.ds(pl.multiple_of(iq * bq + at.start, STRIP), STRIP) for _, at in pieces]
        scores = [_dot(k[keys, _head(i)], q[rows, _head(i)], 1, 1) for (i, _), rows in zip(pieces, asked)]
        ok = gap_s[...] >= j * bk - iq * bq if masked else None
        weights, keeps = [], []
        for (i, at), s in zip(pieces, scores):
            if masked:
                s = jnp.where(ok[:, at], s, HIDDEN)
            old = top_s[i : i + 1, at]
            top = jnp.maximum(old, s.max(axis=0, keepdims=True))
            top_s[i : i + 1, at] = top
            weights.append(jnp.exp2((s - top) * e).astype(LOW))
            keeps.append(jnp.exp2((old - top) * e))
        for (i, at), p, keep in zip(pieces, weights, keeps):
            values = jnp.concatenate([v[keys, _head(i)].T, ones], axis=0)
            mix_s[i, :, at] = mix_s[i, :, at] * keep + _dot(values, p, 1, 0)

    per = bq // bk
    count = width // bq
    total = per * count * (count + 1) // 2

    def attend(n):
        iq = sum((n >= per * i * (i + 1) // 2).astype(jnp.int32) for i in range(1, count))
        j = n - per * iq * (iq + 1) // 2

        @pl.when(j == 0)
        def _():
            top_s[...] = jnp.full_like(top_s, NEG)
            mix_s[...] = jnp.zeros_like(mix_s)

        @pl.when(j < per * iq)
        def _():
            block(iq, j, False)

        @pl.when(j >= per * iq)
        def _():
            block(iq, j, True)

        @pl.when(j == per * (iq + 1) - 1)
        def _():
            rows = pl.ds(pl.multiple_of(iq * bq, bq), bq)
            for i in range(heads):
                top, weight = top_s[i : i + 1, :], mix_s[i, HEAD : HEAD + 1, :]
                out[_head(i), rows] = (mix_s[i, :HEAD, :] * (1 / weight)).astype(LOW)
                lse[i : i + 1, rows] = top * scale + jnp.log(weight)

    def back(ways, g, j, masked):
        keys = pl.ds(pl.multiple_of(j * bk, bk), bk)
        pieces = [(way, i) for way in ways for i in range(heads)]
        qs = [asked_s[way, :, _head(i)] for way, i in pieces]
        dos = [by[g, pl.ds(pl.multiple_of(way * ROWS, ROWS), ROWS), _head(i)] for way, i in pieces]
        scores = [_dot(k[keys, _head(i)], x, 1, 1) for (_, i), x in zip(pieces, qs)]
        dps = [_dot(v[keys, _head(i)], x, 1, 1) for (_, i), x in zip(pieces, dos)]
        for n, (way, i) in enumerate(pieces):
            p = jnp.exp2(scores[n] * e - facts_s[way, i : i + 1, :])
            if masked:
                p = jnp.where(lag_s[...] >= -HALF * way, p, 0.0)
            ds = (p * (dps[n] - facts_s[way, heads + i : heads + i + 1, :])).astype(LOW)
            dv_s[i, keys, :] += _dot(p.astype(LOW), dos[n], 1, 0)
            dk_s[i, keys, :] += _dot(ds, qs[n], 1, 0)
            dq_s[way, i] += _dot(k[keys, _head(i)].T, ds, 1, 0)

    def backward(g):
        begin = starts(g)
        dq_s[...] = jnp.zeros_like(dq_s)
        for n, start in enumerate(begin):
            rows, way = pl.ds(pl.multiple_of(start, HALF), HALF), n // 2
            at = slice(n % 2 * HALF, (n % 2 + 1) * HALF)
            asked_s[way, at, :] = q[rows, :]
            for i in range(heads):
                facts_s[way, i : i + 1, at] = lse[i : i + 1, rows] * LOG2E
                d_out = by[g, n * HALF : (n + 1) * HALF, _head(i)].astype(F32).T
                facts_s[way, heads + i : heads + i + 1, at] = (d_out * out[_head(i), rows].astype(F32)).sum(0, keepdims=True)
        ends = [begins(way, g) for way in range(2)]
        least, most = jnp.minimum(*ends), jnp.maximum(*ends)
        late = (ends[1] > ends[0]).astype(jnp.int32)
        lax.fori_loop(0, least, lambda j, _: back((0, 1), g, j, False), None)
        lax.fori_loop(least, most, lambda j, _: back((late,), g, j, False), None)
        lax.fori_loop(0, 2, lambda way, _: back((way,), g, jnp.where(way == late, most, least), True), None)
        for n, start in enumerate(begin):
            rows, way = pl.ds(pl.multiple_of(start, HALF), HALF), n // 2
            angle = _angle(start // ANGLES, far, near)
            for i in range(heads):
                q[rows, _head(i)] = _turn((dq_s[way, i, :, n % 2 * HALF : (n % 2 + 1) * HALF] * scale).T, angle, 1)

    steps = 2 * CHIPS
    first, share = steps + 1, 4
    began = first + total // share

    def work(m, n, c):
        @pl.when(m == 0)
        def _():
            norm(1)
            loads[1].wait()
            stores[-1].start()
            gap_s[...] = _gap(bk, bq)
            column = lax.broadcasted_iota(jnp.int32, lag_s.shape, 1)
            lag_s[...] = column + jnp.where(column >= HALF, HALF, 0) - lax.broadcasted_iota(jnp.int32, lag_s.shape, 0)
            dk_s[...] = jnp.zeros_like(dk_s)
            dv_s[...] = jnp.zeros_like(dv_s)
            for copy in stores[2:] + loads[2:]:
                copy.wait()

        @pl.when((c == 0) & (n > 0))
        def _():
            for copy in fetch(n - 1):
                copy.wait()

            @pl.when(n <= CHIPS)
            def _():
                project(n - 1)

            @pl.when(n > CHIPS)
            def _():
                products(n - 1)

        @pl.when((c == 1) & (n > 0) & (n <= CHIPS))
        def _():
            turn_over(n - 1)

        @pl.when((m >= first) & (m < began))
        def _():
            lax.fori_loop(share * (m - first), share * (m - first + 1), lambda i, _: attend(i), None)

        @pl.when((m >= began) & ((m <= began + share) | (c == 0)))
        def _():
            backward(jnp.where(m <= began + share, m - began, n - CHIPS - 1))

        @pl.when((c == 1) & (n < steps))
        def _():
            for way in range(2):
                for i in range(2):
                    swap(n // CHIPS, n % CHIPS, way, i, 1 - core).wait_recv()
            for copy in fetch(n):
                copy.start()

    def step(m, _):
        n, c = m // 2, m % 2
        p, g = n // CHIPS, n % CHIPS

        @pl.when((g > 0) & (n < steps))
        def _():
            for way in range(2):
                arrival(p, g, way, c).wait_recv()

        @pl.when((n != CHIPS) & (n < steps - 1))
        def _():
            for way in range(2):
                hop(jnp.where(n == CHIPS - 1, 1, p), jnp.where(n == CHIPS - 1, 0, g), way, c).start()

        @pl.when(n < steps)
        def _():
            for way in range(2):
                swap(p, g, way, c, core).start()

        work(m, n, c)

    lax.fori_loop(0, 2 * steps + 1, step, None)

    def finish(j, _):
        here = pl.ds(pl.multiple_of(j * ANGLES, ANGLES), ANGLES)
        angle = _angle(j, far, near)
        for i in range(heads):
            k[here, _head(i)] = _turn(dk_s[i, here, :] * scale, angle, 1)
            v[here, _head(i)] = dv_s[i, here, :].astype(LOW)

    quarters = [slice(n * QUERIES, (n + 1) * QUERIES) for n in range(count)]
    given = ((out, out_h), (q, dq_h), *((a.at[at, :], b.at[at, :]) for at in quarters for a, b in ((k, dk_h), (v, dv_h))))
    results = [pltpu.make_async_copy(a, b, result_sem.at[n]) for n, (a, b) in enumerate(given)]
    for copy in results[:2]:
        copy.start()
    for n in range(count):
        per = QUERIES // ANGLES
        lax.fori_loop(per * n, per * (n + 1), finish, None)
        for copy in results[2 * n + 2 : 2 * n + 4]:
            copy.start()

    def sent(n, _):
        p, g = n // CHIPS, n % CHIPS
        for way in range(2):
            for c in range(2):
                swap(p, g, way, c, core).wait_send()

                @pl.when(g < CHIPS - 1)
                def _():
                    hop(p, g, way, c).wait_send()

    lax.fori_loop(0, steps, sent, None)
    for copy in put(CHIPS - 1):
        copy.wait()
    for copy in results:
        copy.wait()


def gather(x, dy, gain, wq, wk, wv, wo, far, near):
    width, rows = x.shape[1], GROUP * ROWS
    heads = ROWS // HEAD
    vmem, dma = pltpu.VMEM, pltpu.SemaphoreType.DMA
    here = pl.BlockSpec(memory_space=pltpu.VMEM)
    by_token, by_head, sums = (rows, ROWS), (ROWS, rows), (heads, rows, HEAD)
    shapes = [(2, rows, width), (width, rows), by_token, by_token, by_token, by_head]
    return pl.pallas_call(
        _gather,
        in_specs=[ANY, ANY, here, ANY, ANY, ANY, ANY, here, here],
        out_specs=[ANY] * len(shapes),
        out_shape=[jax.ShapeDtypeStruct(shape, LOW) for shape in shapes],
        scratch_shapes=[
            vmem(x.shape, LOW), vmem(x.shape, LOW), vmem((width, 3 * ROWS), LOW), vmem((ROWS, width), LOW), vmem((2, SPAN, width), LOW),
            vmem((width, SPAN), LOW), *[vmem(by_token, LOW)] * 3, vmem((CHIPS, SPAN, ROWS), LOW), vmem(by_head, LOW), vmem((heads, rows), F32),
            vmem((heads, QUERIES), F32), vmem((heads, HEAD + 8, QUERIES), F32), vmem((KEYS, QUERIES), jnp.int32),
            vmem((2, ROWS, ROWS), LOW), vmem((2, 2 * heads, ROWS), F32), vmem((2, heads, HEAD, ROWS), F32), vmem(sums, F32), vmem(sums, F32),
            vmem((KEYS, ROWS), jnp.int32),
            dma((6,)), dma((5,)), *[dma((2, CHIPS, 2, 2))] * 4, dma((2, 4)), dma((4,)), dma((10,)),
        ],
        compiler_params=pltpu.CompilerParams(collective_id=1, has_side_effects=True, vmem_limit_bytes=VMEM),
        cost_estimate=pl.CostEstimate(flops=2 * rows * width * ROWS * 8, transcendentals=rows * rows, bytes_accessed=rows * width * 8),
    )(x, dy, gain, wq, wk, wv, wo, far, near)

def solution(mesh):
    def step(x, dy, gain, wq, wk, wv, wo):
        gain = gain[None]
        far, near = tables(GROUP * ROWS)
        gathered, at, dq, dk, dv, out = gather(x, dy, gain, wq, wk, wv, wo, far, near)
        return tuple(keep(scatter(dq, dk, dv, wq, wk, wv, at, gathered, out, x, dy, gain)))

    tokens, columns = P(("dp", "tp"), None), P(None, "tp")
    return jax.shard_map(
        step,
        mesh=mesh,
        in_specs=(tokens, tokens, P(None), columns, columns, columns, P("tp", None)),
        out_specs=(tokens, P("dp", None), P("dp", "tp"), P("dp", "tp"), P("dp", "tp"), P(("dp", "tp"), None)),
        check_vma=False,
    )
```
